16 devices in a mesh: q: 16 (over z, y, x, core).
Axes of the slice: x: 2, y: 2, z: 2, core: 2. Of those that a mesh axis runs over, the one named last changes fastest.
Arguments:
- state_in: float32 [2, 33554432], P(None, 'q')
- unitaries: float32 [2, 25, 2, 2], replicated
- cz_pairs: int32 [12, 2], replicated
Outputs:
- output 1: float32 [2, 33554432], P(None, 'q')
- output 2: float32 [25], replicated
All inputs are finite; a program needn't handle non-finite values.
Results may differ from the reference program's by a relative error of at most 0.001.
Values sent between devices are 32-bit elements.
A program may use at most 1 GiB of HBM per device.

```python
import math
import jax
import jax.numpy as jnp
from jax import lax

QUBITS = 25
NUM_PAIRS = QUBITS // 2
STATE_SIZE = 2 ** QUBITS


def u3_gates(theta_angle, phi_angle, lam_angle):
    cos_half = jnp.cos(0.5 * theta_angle)
    sin_half = jnp.sin(0.5 * theta_angle)
    zero_part = jnp.zeros_like(cos_half)
    real_part = jnp.stack([
        jnp.stack([cos_half, -jnp.cos(lam_angle) * sin_half], axis=-1),
        jnp.stack([jnp.cos(phi_angle) * sin_half, jnp.cos(phi_angle + lam_angle) * cos_half], axis=-1)], axis=-2)
    imag_part = jnp.stack([
        jnp.stack([zero_part, -jnp.sin(lam_angle) * sin_half], axis=-1),
        jnp.stack([jnp.sin(phi_angle) * sin_half, jnp.sin(phi_angle + lam_angle) * cos_half], axis=-1)], axis=-2)
    return jnp.stack([real_part, imag_part])


def product_envelope(zero_weight, env_angle):
    env_re = jnp.ones((1,), jnp.float32)
    env_im = jnp.zeros((1,), jnp.float32)
    for qubit_pos in range(QUBITS):
        amp_zero = jnp.sqrt(2.0 * zero_weight[qubit_pos])
        amp_one = jnp.sqrt(2.0 * (1.0 - zero_weight[qubit_pos]))
        fac_re = jnp.stack([amp_zero, amp_one * jnp.cos(env_angle[qubit_pos])])
        fac_im = jnp.stack([jnp.zeros_like(amp_zero), amp_one * jnp.sin(env_angle[qubit_pos])])
        next_re = (env_re[:, None] * fac_re[None, :] - env_im[:, None] * fac_im[None, :]).reshape(-1)
        next_im = (env_re[:, None] * fac_im[None, :] + env_im[:, None] * fac_re[None, :]).reshape(-1)
        env_re = next_re
        env_im = next_im
    return env_re, env_im


def setup_inputs(seed: int = 0) -> dict:
    root_key = jax.random.key(seed)
    key_amp, key_bias, key_theta, key_phase, key_pairs, key_env = jax.random.split(root_key, 6)
    zero_weight = jax.random.uniform(key_bias, (QUBITS,), jnp.float32, 0.15, 0.85)
    env_angle = jax.random.uniform(key_env, (QUBITS,), jnp.float32, 0.0, 2.0 * math.pi)
    env_re, env_im = product_envelope(zero_weight, env_angle)
    noise = 0.6 * jax.random.normal(key_amp, (2, STATE_SIZE), jnp.float32)
    base_re = 1.0 + noise[0]
    base_im = noise[1]
    amplitudes = jnp.stack([env_re * base_re - env_im * base_im, env_re * base_im + env_im * base_re])
    amplitudes = amplitudes * lax.rsqrt(jnp.mean(jnp.sum(amplitudes * amplitudes, axis=0)))
    theta_angle = jax.random.uniform(key_theta, (QUBITS,), jnp.float32, 0.35 * math.pi, 0.65 * math.pi)
    phase_angle = jax.random.uniform(key_phase, (2, QUBITS), jnp.float32, 0.0, 2.0 * math.pi)
    unitaries = u3_gates(theta_angle, phase_angle[0], phase_angle[1])
    cz_pairs = jax.random.permutation(key_pairs, QUBITS)[: 2 * NUM_PAIRS].reshape(NUM_PAIRS, 2).astype(jnp.int32)
    return {'state_in': amplitudes, 'unitaries': unitaries, 'cz_pairs': cz_pairs}


def mix_pair(first, second, coef_a, coef_b):
    out_re = coef_a[0] * first[0] - coef_a[1] * first[1] + coef_b[0] * second[0] - coef_b[1] * second[1]
    out_im = coef_a[0] * first[1] + coef_a[1] * first[0] + coef_b[0] * second[1] + coef_b[1] * second[0]
    return jnp.stack([out_re, out_im])


def apply_gate(state, bit_pos, gate_mat):
    view = state.reshape(2, 2 ** bit_pos, 2, -1)
    zero_half = view[:, :, 0, :]
    one_half = view[:, :, 1, :]
    new_zero = mix_pair(zero_half, one_half, gate_mat[:, 0, 0], gate_mat[:, 0, 1])
    new_one = mix_pair(zero_half, one_half, gate_mat[:, 1, 0], gate_mat[:, 1, 1])
    return jnp.stack([new_zero, new_one], axis=2).reshape(state.shape)


def pair_signs(flat_index, cz_pairs):
    parity = jnp.zeros_like(flat_index)
    for pair_pos in range(NUM_PAIRS):
        shift_a = QUBITS - 1 - cz_pairs[pair_pos, 0]
        shift_b = QUBITS - 1 - cz_pairs[pair_pos, 1]
        parity = parity ^ ((flat_index >> shift_a) & (flat_index >> shift_b) & 1)
    return (1 - 2 * parity).astype(jnp.float32)


def reference(state_in, unitaries, cz_pairs):
    state = state_in
    for qubit_pos in range(QUBITS):
        state = apply_gate(state, qubit_pos, unitaries[:, qubit_pos])
    flat_index = lax.iota(jnp.int32, STATE_SIZE)
    state = state * pair_signs(flat_index, cz_pairs)[None, :]
    density = state[0] * state[0] + state[1] * state[1]
    halves = [jnp.sum(density.reshape(2 ** qubit_pos, 2, -1), axis=(0, 2)) for qubit_pos in range(QUBITS)]
    z_expect = jnp.stack([bit_sums[0] - bit_sums[1] for bit_sums in halves]) / STATE_SIZE
    return state, z_expect
```

```python
import functools
import jax
import jax.numpy as jnp
from jax import lax
from jax.experimental import pallas as pl
from jax.experimental.pallas import tpu as pltpu
from jax.sharding import PartitionSpec as P

MESH = pl.DeviceIdType.MESH
LANES = 128
LANE_BITS = 7
ROW_BITS = 7
MID_BITS = 5
QUARTERS = 4
BLOCKS = 2 ** MID_BITS
BLOCK_ROWS = 2 * 2 ** ROW_BITS
HALF = BLOCK_ROWS // 2
STEPS = 16
STEP_BLOCKS = BLOCKS // STEPS
TOP_BITS = 4
CORE = 3
HI_BITS = 2 + MID_BITS
HIGHEST = lax.Precision.HIGHEST


def apply_coefs(coef_a, coef_b, first, second):
    out_re = coef_a[0] * first[0] - coef_a[1] * first[1] + coef_b[0] * second[0] - coef_b[1] * second[1]
    out_im = coef_a[0] * first[1] + coef_a[1] * first[0] + coef_b[0] * second[1] + coef_b[1] * second[0]
    return out_re, out_im


def gate_coefs(gates_ref, qubit):
    return [[(gates_ref[0, row, col, qubit], gates_ref[1, row, col, qubit]) for col in range(2)] for row in range(2)]


def butterfly(values, gates):
    size = len(values)
    for gate_pos, gate in enumerate(gates):
        stride = size >> (gate_pos + 1)
        values = list(values)
        for pos in range(size):
            if pos & stride:
                continue
            zero_half, one_half = values[pos], values[pos + stride]
            values[pos] = apply_coefs(gate[0][0], gate[0][1], zero_half, one_half)
            values[pos + stride] = apply_coefs(gate[1][0], gate[1][1], zero_half, one_half)
    return values


def load_rows(ref, row, rows):
    return ref[pl.ds(2 * row, rows, stride=2), :], ref[pl.ds(2 * row + 1, rows, stride=2), :]


def store_rows(ref, row, rows, value):
    ref[pl.ds(2 * row, rows, stride=2), :] = value[0]
    ref[pl.ds(2 * row + 1, rows, stride=2), :] = value[1]


def gate_blocks(refs, gates, rows):
    @pl.loop(0, HALF // rows)
    def _(group):
        row = pl.multiple_of(group * rows, rows)
        values = butterfly([load_rows(ref, row, rows) for ref in refs], gates)
        for ref, value in zip(refs, values):
            store_rows(ref, row, rows, value)


def build_matrix(mat_ref, gates_ref, first_qubit, num_bits, transposed):
    size = 2 ** num_bits
    out_index = lax.broadcasted_iota(jnp.int32, (size, size), 1 if transposed else 0)
    in_index = lax.broadcasted_iota(jnp.int32, (size, size), 0 if transposed else 1)
    prod_re = jnp.ones((size, size), jnp.float32)
    prod_im = jnp.zeros((size, size), jnp.float32)
    for bit_pos in range(num_bits):
        gate = gate_coefs(gates_ref, first_qubit + bit_pos)
        mask = 2 ** (num_bits - 1 - bit_pos)
        out_one = (out_index & mask) != 0
        in_one = (in_index & mask) != 0
        fac_re, fac_im = [jnp.where(out_one, jnp.where(in_one, gate[1][1][part], gate[1][0][part]), jnp.where(in_one, gate[0][1][part], gate[0][0][part])) for part in range(2)]
        prod_re, prod_im = prod_re * fac_re - prod_im * fac_im, prod_re * fac_im + prod_im * fac_re
    mat_ref[0:size, 0:size] = prod_re
    mat_ref[size:, size:] = prod_re
    mat_ref[0:size, size:] = prod_im if transposed else -prod_im
    mat_ref[size:, 0:size] = -prod_im if transposed else prod_im


def kernel(group_size, x_ref, gates_ref, pairs_ref, out_ref, z_ref, recv_ref, lane_mat, row_mat, low_sum, high_sum, part_ref, parts_ref,
           mask_ref, load_sem, send_sem, recv_sem, part_send, part_recv):
    num_qubits = gates_ref.shape[3]
    num_pairs = pairs_ref.shape[1]
    me = lax.axis_index('q')
    strides = [group_size >> (link + 1) for link in range(TOP_BITS)]
    own_bits = [(me // stride) % 2 for stride in strides]
    partners = [me + stride * (1 - 2 * own_bit) for stride, own_bit in zip(strides, own_bits)]

    def blocks_of(quarter, step):
        return out_ref.at[quarter, pl.ds(step * STEP_BLOCKS, STEP_BLOCKS)]

    def load(step):
        span = pl.ds(step * STEP_BLOCKS, STEP_BLOCKS)
        return pltpu.make_async_copy(x_ref.at[:, span], out_ref.at[:, span], load_sem.at[step])

    def exchange(link, slot, step):
        return pltpu.make_async_remote_copy(
            src_ref=blocks_of((slot + link) % 4, step), dst_ref=recv_ref.at[link, slot % 2, pl.ds(step * STEP_BLOCKS, STEP_BLOCKS)],
            send_sem=send_sem.at[link, step], recv_sem=recv_sem.at[link, slot % 2, step],
            device_id=(partners[link],), device_id_type=MESH)

    def send_links(slot, step):
        for link in range(CORE):
            exchange(link, slot, step).start()

    @pl.loop(0, STEPS)
    def _(step):
        load(step).start()

    barrier = pltpu.get_barrier_semaphore()
    for offset in range(1, group_size):
        pl.semaphore_signal(barrier, inc=1, device_id=((me + offset) % group_size,), device_id_type=MESH)

    for pair_pos in range(num_pairs):
        mask_ref[pair_pos] = (1 << (num_qubits - 1 - pairs_ref[0, pair_pos])) | (1 << (num_qubits - 1 - pairs_ref[1, pair_pos]))
    low_sum[...] = jnp.zeros_like(low_sum)
    high_sum[...] = jnp.zeros_like(high_sum)
    pl.semaphore_wait(barrier, group_size - 1)

    quarter_gates = [gate_coefs(gates_ref, TOP_BITS), gate_coefs(gates_ref, TOP_BITS + 1)]

    @pl.loop(0, STEPS)
    def _(step):
        @pl.when(step > 0)
        def _():
            send_links(0, step - 1)

        load(step).wait()
        for block in range(STEP_BLOCKS):
            gate_blocks([out_ref.at[quarter, step * STEP_BLOCKS + block] for quarter in range(QUARTERS)], quarter_gates, 16)

    def mid_gates(quarter):
        first = TOP_BITS + 2
        gates = [gate_coefs(gates_ref, first + bit_pos) for bit_pos in range(MID_BITS)]

        @pl.loop(0, BLOCKS // 8)
        def _(low):
            gate_blocks([out_ref.at[quarter, pos * (BLOCKS // 8) + low] for pos in range(8)], gates[:3], 8)

        @pl.loop(0, BLOCKS // 4)
        def _(high):
            gate_blocks([out_ref.at[quarter, high * 4 + pos] for pos in range(4)], gates[3:], 16)

    def finish(quarter, block, row, rows, value):
        first_row = ((me * QUARTERS + quarter) * BLOCKS + block) * HALF + row
        index = first_row * LANES + lax.broadcasted_iota(jnp.int32, (rows, LANES), 0) * LANES + lax.broadcasted_iota(jnp.int32, (rows, LANES), 1)
        odd = None
        for pair_pos in range(num_pairs):
            mask = mask_ref[pair_pos]
            hit = (index & mask) == mask
            odd = hit if odd is None else jnp.logical_xor(odd, hit)
        sign = jnp.where(odd, -1.0, 1.0)
        value = (value[0] * sign, value[1] * sign)
        store_rows(out_ref.at[quarter, block], row, rows, value)
        density = value[0] * value[0] + value[1] * value[1]
        low_sum[pl.ds(row, rows), :] += density
        return jnp.sum(density.reshape(rows // 8, 8, LANES), axis=0)

    def add_high(quarter, block, total):
        position = quarter * BLOCKS + block
        for bit_pos in range(HI_BITS):
            bit = (position // 2 ** (HI_BITS - 1 - bit_pos)) % 2
            high_sum[bit_pos] += total * (1 - 2 * bit).astype(jnp.float32)
        high_sum[HI_BITS] += total

    def mix(link, slot, step, last):
        quarter = (slot + link) % 4
        own_bit = own_bits[link]
        coef_self = [gates_ref[part, own_bit, own_bit, link] for part in range(2)]
        coef_other = [gates_ref[part, own_bit, 1 - own_bit, link] for part in range(2)]
        rows = 32
        for step_block in range(STEP_BLOCKS):
            block = step * STEP_BLOCKS + step_block
            own_ref = out_ref.at[quarter, block]
            other_ref = recv_ref.at[link, slot % 2, block]

            def body(group, total):
                row = pl.multiple_of(group * rows, rows)
                value = apply_coefs(coef_self, coef_other, load_rows(own_ref, row, rows), load_rows(other_ref, row, rows))
                if last:
                    return total + finish(quarter, block, row, rows, value)
                store_rows(own_ref, row, rows, value)
                return total

            total = lax.fori_loop(0, HALF // rows, body, jnp.zeros((8, LANES), jnp.float32))
            if last:
                add_high(quarter, block, total)

    def local(slot, step, last):
        quarter = (slot + CORE) % 4
        copy = exchange(CORE, slot, step)
        copy.wait_recv()
        copy.wait_send()
        mix(CORE, slot, step, False)
        refs = [out_ref.at[quarter, step * STEP_BLOCKS + block] for block in range(STEP_BLOCKS)]
        parts = [load_rows(ref, 0, HALF) for ref in refs]
        rows = jnp.concatenate([jnp.concatenate(part, axis=1) for part in parts], axis=0)
        mixed = jnp.dot(rows, lane_mat[...], precision=HIGHEST, preferred_element_type=jnp.float32)
        columns = jnp.concatenate([
            jnp.concatenate([mixed[block * HALF:(block + 1) * HALF, :LANES], mixed[block * HALF:(block + 1) * HALF, LANES:]], axis=0)
            for block in range(STEP_BLOCKS)], axis=1)
        done = jnp.dot(row_mat[...], columns, precision=HIGHEST, preferred_element_type=jnp.float32)
        for block, ref in enumerate(refs):
            piece = done[:, block * LANES:(block + 1) * LANES]
            store_rows(ref, 0, HALF, (piece[:HALF], piece[HALF:]))
        if last:
            rows_now = 32
            for step_block in range(STEP_BLOCKS):
                block = step * STEP_BLOCKS + step_block

                def body(group, total):
                    row = pl.multiple_of(group * rows_now, rows_now)
                    return total + finish(quarter, block, row, rows_now, load_rows(out_ref.at[quarter, block], row, rows_now))

                total = lax.fori_loop(0, HALF // rows_now, body, jnp.zeros((8, LANES), jnp.float32))
                add_high(quarter, block, total)

    for slot in range(QUARTERS):
        mid_gates((slot + CORE) % 4)
        send_links(slot, STEPS - 1)

        @pl.loop(0, STEPS)
        def _(step):
            exchange(CORE, slot, step).start()

        if slot == 0:
            build_matrix(lane_mat, gates_ref, num_qubits - LANE_BITS, LANE_BITS, True)
            build_matrix(row_mat, gates_ref, num_qubits - LANE_BITS - ROW_BITS, ROW_BITS, False)
        last = slot == QUARTERS - 1

        @pl.loop(0, STEPS)
        def _(step):
            if not last:
                @pl.when(step > 0)
                def _():
                    send_links(slot + 1, step - 1)
            local(slot, step, last)
            for link in range(CORE):
                copy = exchange(link, slot, step)
                copy.wait_recv()
                copy.wait_send()
                mix(link, slot, step, last)

    total = high_sum[HI_BITS]
    sublane = lax.broadcasted_iota(jnp.int32, (8, LANES), 0)
    lane = lax.broadcasted_iota(jnp.int32, (8, LANES), 1)
    signed = [total * (1 - 2 * own_bit).astype(jnp.float32) for own_bit in own_bits]
    signed += [high_sum[bit_pos] for bit_pos in range(HI_BITS)]
    low = [low_sum[8 * pos:8 * pos + 8, :] for pos in range(HALF // 8)]
    for bit_pos in range(ROW_BITS - 3):
        mask = 2 ** (ROW_BITS - 4 - bit_pos)
        signed.append(functools.reduce(jnp.add, [-part if pos & mask else part for pos, part in enumerate(low)]))
    signed += [jnp.where((sublane & (4 >> bit_pos)) != 0, -total, total) for bit_pos in range(3)]
    signed += [jnp.where((lane & (64 >> bit_pos)) != 0, -total, total) for bit_pos in range(LANE_BITS)]
    rows = [jnp.sum(part, axis=0, keepdims=True) for part in signed]
    table = jnp.concatenate(rows + [jnp.zeros((LANES - len(rows), LANES), jnp.float32)], axis=0)
    part = lax.dot_general(jnp.ones((8, LANES), jnp.float32), table, (((1,), (1,)), ((), ())), precision=HIGHEST, preferred_element_type=jnp.float32)
    part_ref[...] = part

    def share(offset):
        return pltpu.make_async_remote_copy(
            src_ref=part_ref, dst_ref=parts_ref.at[me], send_sem=part_send.at[offset], recv_sem=part_recv.at[me],
            device_id=((me + offset) % group_size,), device_id_type=MESH)

    def shared(offset):
        source = (me + group_size - offset) % group_size
        return pltpu.make_async_remote_copy(
            src_ref=part_ref, dst_ref=parts_ref.at[source], send_sem=part_send.at[offset], recv_sem=part_recv.at[source],
            device_id=((me + offset) % group_size,), device_id_type=MESH)

    for offset in range(1, group_size):
        share(offset).start()
    parts_ref[me] = part
    for offset in range(1, group_size):
        shared(offset).wait_recv()
    for offset in range(1, group_size):
        share(offset).wait_send()
    z_ref[...] = functools.reduce(jnp.add, [parts_ref[pos] for pos in range(group_size)]) * (1.0 / 2 ** num_qubits)


def solution(mesh):
    group_size = mesh.shape['q']

    def local_layer(state_local, unitaries, cz_pairs):
        num_qubits = unitaries.shape[1]
        local_size = state_local.shape[1]
        row_count = local_size // LANES
        shape = (QUARTERS, BLOCKS, BLOCK_ROWS, LANES)
        grid = state_local.reshape(2, row_count, LANES).transpose(1, 0, 2).reshape(shape)
        state, sums = pl.pallas_call(
            functools.partial(kernel, group_size),
            out_shape=(pltpu.VMEM(shape, jnp.float32), jax.ShapeDtypeStruct((8, LANES), jnp.float32)),
            in_specs=[pl.BlockSpec(memory_space=pl.ANY), pl.BlockSpec(memory_space=pltpu.SMEM), pl.BlockSpec(memory_space=pltpu.SMEM)],
            out_specs=(pl.BlockSpec(memory_space=pltpu.VMEM), pl.BlockSpec(memory_space=pltpu.VMEM)),
            scratch_shapes=[
                pltpu.VMEM((TOP_BITS, 2, BLOCKS, BLOCK_ROWS, LANES), jnp.float32),
                pltpu.VMEM((2 * LANES, 2 * LANES), jnp.float32),
                pltpu.VMEM((BLOCK_ROWS, BLOCK_ROWS), jnp.float32),
                pltpu.VMEM((HALF, LANES), jnp.float32),
                pltpu.VMEM((HI_BITS + 1, 8, LANES), jnp.float32),
                pltpu.VMEM((8, LANES), jnp.float32),
                pltpu.VMEM((group_size, 8, LANES), jnp.float32),
                pltpu.SMEM((cz_pairs.shape[0],), jnp.int32),
                pltpu.SemaphoreType.DMA((STEPS,)),
                pltpu.SemaphoreType.DMA((TOP_BITS, STEPS)),
                pltpu.SemaphoreType.DMA((TOP_BITS, 2, STEPS)),
                pltpu.SemaphoreType.DMA((group_size,)),
                pltpu.SemaphoreType.DMA((group_size,)),
            ],
            compiler_params=pltpu.CompilerParams(collective_id=0, has_side_effects=True, vmem_limit_bytes=44 * 1024 * 1024),
        )(grid, unitaries.transpose(0, 2, 3, 1), cz_pairs.T)
        state = state.reshape(row_count, 2, LANES).transpose(1, 0, 2).reshape(2, local_size)
        return state, sums[0, :num_qubits]

    return jax.shard_map(local_layer, mesh=mesh, in_specs=(P(None, 'q'), P(), P()), out_specs=(P(None, 'q'), P()), check_vma=False)
```

```python
import functools
import jax
import jax.numpy as jnp
from jax import lax
from jax.experimental import pallas as pl
from jax.experimental.pallas import tpu as pltpu
from jax.sharding import PartitionSpec as P

MESH = pl.DeviceIdType.MESH
LANES = 128
LANE_BITS = 7
ROW_BITS = 7
MID_BITS = 5
QUARTERS = 4
BLOCKS = 2 ** MID_BITS
BLOCK_ROWS = 2 * 2 ** ROW_BITS
HALF = BLOCK_ROWS // 2
LOCAL_BLOCKS = 2
LOAD_SPANS = (1, 6, 9, 16)
LINK_SPANS = ((1, 6, 9, 16), (16, 16), (16, 16), (16, 11, 4, 1))
CORE_SPANS = (8, 8, 8, 8)
MAX_PIECES = 4
FLUSH_PIECES = 1
TOP_BITS = 4
CORE = 3
HI_BITS = 2 + MID_BITS
HIGHEST = lax.Precision.HIGHEST


def apply_coefs(coef_a, coef_b, first, second):
    out_re = coef_a[0] * first[0] - coef_a[1] * first[1] + coef_b[0] * second[0] - coef_b[1] * second[1]
    out_im = coef_a[0] * first[1] + coef_a[1] * first[0] + coef_b[0] * second[1] + coef_b[1] * second[0]
    return out_re, out_im


def gate_coefs(gates_ref, qubit):
    return [[(gates_ref[0, row, col, qubit], gates_ref[1, row, col, qubit]) for col in range(2)] for row in range(2)]


def pieces_of(spans):
    starts = [sum(spans[:pos]) for pos in range(len(spans))]
    return list(zip(starts, spans))


def butterfly(values, gates):
    size = len(values)
    for gate_pos, gate in enumerate(gates):
        stride = size >> (gate_pos + 1)
        values = list(values)
        for pos in range(size):
            if pos & stride:
                continue
            zero_half, one_half = values[pos], values[pos + stride]
            values[pos] = apply_coefs(gate[0][0], gate[0][1], zero_half, one_half)
            values[pos + stride] = apply_coefs(gate[1][0], gate[1][1], zero_half, one_half)
    return values


def load_rows(ref, row, rows):
    return ref[pl.ds(2 * row, rows, stride=2), :], ref[pl.ds(2 * row + 1, rows, stride=2), :]


def store_rows(ref, row, rows, value):
    ref[pl.ds(2 * row, rows, stride=2), :] = value[0]
    ref[pl.ds(2 * row + 1, rows, stride=2), :] = value[1]


def gate_blocks(refs, gates, rows):
    @pl.loop(0, HALF // rows)
    def _(group):
        row = pl.multiple_of(group * rows, rows)
        values = butterfly([load_rows(ref, row, rows) for ref in refs], gates)
        for ref, value in zip(refs, values):
            store_rows(ref, row, rows, value)


def build_matrix(mat_ref, gates_ref, first_qubit, num_bits, transposed):
    size = 2 ** num_bits
    out_index = lax.broadcasted_iota(jnp.int32, (size, size), 1 if transposed else 0)
    in_index = lax.broadcasted_iota(jnp.int32, (size, size), 0 if transposed else 1)
    prod_re = jnp.ones((size, size), jnp.float32)
    prod_im = jnp.zeros((size, size), jnp.float32)
    for bit_pos in range(num_bits):
        gate = gate_coefs(gates_ref, first_qubit + bit_pos)
        mask = 2 ** (num_bits - 1 - bit_pos)
        out_one = (out_index & mask) != 0
        in_one = (in_index & mask) != 0
        fac_re, fac_im = [jnp.where(out_one, jnp.where(in_one, gate[1][1][part], gate[1][0][part]), jnp.where(in_one, gate[0][1][part], gate[0][0][part])) for part in range(2)]
        prod_re, prod_im = prod_re * fac_re - prod_im * fac_im, prod_re * fac_im + prod_im * fac_re
    mat_ref[0:size, 0:size] = prod_re
    mat_ref[size:, size:] = prod_re
    mat_ref[0:size, size:] = prod_im if transposed else -prod_im
    mat_ref[size:, 0:size] = -prod_im if transposed else prod_im


def kernel(group_size, x_ref, gates_hbm, pairs_hbm, out_ref, parts_ref, recv_ref, lane_mat, row_mat, low_sum, high_sum, part_ref,
           gates_ref, pairs_ref, mask_ref, small_sem, ready_sem, load_sem, send_sem, recv_sem, part_send, part_recv):
    num_qubits = gates_hbm.shape[3]
    num_pairs = pairs_hbm.shape[1]
    me = lax.axis_index('q')
    strides = [group_size >> (link + 1) for link in range(TOP_BITS)]
    own_bits = [(me // stride) % 2 for stride in strides]
    partners = [me + stride * (1 - 2 * own_bit) for stride, own_bit in zip(strides, own_bits)]

    load_pieces = pieces_of(LOAD_SPANS)
    link_pieces = [pieces_of(spans) for spans in LINK_SPANS]
    core_pieces = pieces_of(CORE_SPANS)

    def load(piece):
        span = pl.ds(*load_pieces[piece])
        return pltpu.make_async_copy(x_ref.at[:, span], out_ref.at[:, span], load_sem.at[piece])

    def exchange(link, slot, piece):
        span = pl.ds(*(core_pieces if link == CORE else link_pieces[slot])[piece])
        return pltpu.make_async_remote_copy(
            src_ref=out_ref.at[(slot + link) % 4, span], dst_ref=recv_ref.at[link, slot % 2, span],
            send_sem=send_sem.at[link, slot % 2, piece], recv_sem=recv_sem.at[link, slot % 2, piece],
            device_id=(partners[link],), device_id_type=MESH)

    def send_links(slot, done_from, done_to):
        for piece, (start, size) in enumerate(link_pieces[slot]):
            if done_from < start + size <= done_to:
                for link in range(CORE):
                    exchange(link, slot, piece).start()

    barrier = pltpu.get_barrier_semaphore()
    for partner in partners:
        pl.semaphore_signal(barrier, inc=1, device_id=(partner,), device_id_type=MESH)
    small = [pltpu.make_async_copy(gates_hbm, gates_ref, small_sem.at[0]), pltpu.make_async_copy(pairs_hbm, pairs_ref, small_sem.at[1])]
    load(0).start()
    for copy in small:
        copy.start()
    for piece in range(1, len(load_pieces)):
        load(piece).start()
    for copy in small:
        copy.wait()

    quarter_gates = [gate_coefs(gates_ref, TOP_BITS), gate_coefs(gates_ref, TOP_BITS + 1)]

    for piece, (start, size) in enumerate(load_pieces):
        load(piece).wait()

        @pl.loop(start, start + size)
        def _(block):
            gate_blocks([out_ref.at[quarter, block] for quarter in range(QUARTERS)], quarter_gates, 16)

        if piece == 0:
            pl.semaphore_wait(barrier, TOP_BITS)
        send_links(0, start, start + size)

    def mid_gates(quarter):
        first = TOP_BITS + 2
        gates = [gate_coefs(gates_ref, first + bit_pos) for bit_pos in range(MID_BITS)]

        @pl.loop(0, BLOCKS // 8)
        def _(low):
            gate_blocks([out_ref.at[quarter, pos * (BLOCKS // 8) + low] for pos in range(8)], gates[:3], 8)

        @pl.loop(0, BLOCKS // 4)
        def _(high):
            gate_blocks([out_ref.at[quarter, high * 4 + pos] for pos in range(4)], gates[3:], 16)

    def finish(quarter, block, row, rows, value):
        first_row = ((me * QUARTERS + quarter) * BLOCKS + block) * HALF + row
        index = first_row * LANES + lax.broadcasted_iota(jnp.int32, (rows, LANES), 0) * LANES + lax.broadcasted_iota(jnp.int32, (rows, LANES), 1)
        odd = None
        for pair_pos in range(num_pairs):
            mask = mask_ref[pair_pos]
            hit = (index & mask) == mask
            odd = hit if odd is None else jnp.logical_xor(odd, hit)
        sign = jnp.where(odd, -1.0, 1.0)
        value = (value[0] * sign, value[1] * sign)
        store_rows(out_ref.at[quarter, block], row, rows, value)
        density = value[0] * value[0] + value[1] * value[1]
        low_sum[pl.ds(row, rows), :] += density
        return jnp.sum(density.reshape(rows // 8, 8, LANES), axis=0)

    def add_high(quarter, block, total):
        position = quarter * BLOCKS + block
        for bit_pos in range(HI_BITS):
            bit = (position // 2 ** (HI_BITS - 1 - bit_pos)) % 2
            high_sum[bit_pos] += total * (1 - 2 * bit).astype(jnp.float32)
        high_sum[HI_BITS] += total

    def mix(link, slot, block, last):
        quarter = (slot + link) % 4
        own_bit = own_bits[link]
        coef_self = [gates_ref[part, own_bit, own_bit, link] for part in range(2)]
        coef_other = [gates_ref[part, own_bit, 1 - own_bit, link] for part in range(2)]
        rows = 32
        own_ref = out_ref.at[quarter, block]
        other_ref = recv_ref.at[link, slot % 2, block]

        def body(group, total):
            row = pl.multiple_of(group * rows, rows)
            value = apply_coefs(coef_self, coef_other, load_rows(own_ref, row, rows), load_rows(other_ref, row, rows))
            if last:
                return total + finish(quarter, block, row, rows, value)
            store_rows(own_ref, row, rows, value)
            return total

        total = lax.fori_loop(0, HALF // rows, body, jnp.zeros((8, LANES), jnp.float32))
        if last:
            add_high(quarter, block, total)

    def local(slot, first_block, last):
        quarter = (slot + CORE) % 4
        blocks = [first_block + pos for pos in range(LOCAL_BLOCKS)]
        for block in blocks:
            mix(CORE, slot, block, False)
        refs = [out_ref.at[quarter, block] for block in blocks]
        parts = [load_rows(ref, 0, HALF) for ref in refs]
        rows = jnp.concatenate([jnp.concatenate(part, axis=1) for part in parts], axis=0)
        mixed = jnp.dot(rows, lane_mat[...], precision=HIGHEST, preferred_element_type=jnp.float32)
        columns = jnp.concatenate([
            jnp.concatenate([mixed[pos * HALF:(pos + 1) * HALF, :LANES], mixed[pos * HALF:(pos + 1) * HALF, LANES:]], axis=0)
            for pos in range(LOCAL_BLOCKS)], axis=1)
        done = jnp.dot(row_mat[...], columns, precision=HIGHEST, preferred_element_type=jnp.float32)
        for pos, ref in enumerate(refs):
            piece = done[:, pos * LANES:(pos + 1) * LANES]
            store_rows(ref, 0, HALF, (piece[:HALF], piece[HALF:]))
        if last:
            group_rows = 32
            for block in blocks:
                def body(group, total):
                    row = pl.multiple_of(group * group_rows, group_rows)
                    return total + finish(quarter, block, row, group_rows, load_rows(out_ref.at[quarter, block], row, group_rows))

                total = lax.fori_loop(0, HALF // group_rows, body, jnp.zeros((8, LANES), jnp.float32))
                add_high(quarter, block, total)

    for pair_pos in range(num_pairs):
        mask_ref[pair_pos] = (1 << (num_qubits - 1 - pairs_ref[0, pair_pos])) | (1 << (num_qubits - 1 - pairs_ref[1, pair_pos]))
    low_sum[...] = jnp.zeros_like(low_sum)
    high_sum[...] = jnp.zeros_like(high_sum)
    for link, partner in enumerate(partners):
        pl.semaphore_signal(ready_sem.at[link], inc=1, device_id=(partner,), device_id_type=MESH)
        pl.semaphore_wait(ready_sem.at[link], 1)
    build_matrix(lane_mat, gates_ref, num_qubits - LANE_BITS, LANE_BITS, True)
    build_matrix(row_mat, gates_ref, num_qubits - LANE_BITS - ROW_BITS, ROW_BITS, False)
    for slot in range(QUARTERS):
        last = slot == QUARTERS - 1
        mid_gates((slot + CORE) % 4)
        for piece in range(len(core_pieces)):
            exchange(CORE, slot, piece).start()
        for piece, (start, size) in enumerate(core_pieces):
            copy = exchange(CORE, slot, piece)
            copy.wait_recv()
            copy.wait_send()

            @pl.loop(start // LOCAL_BLOCKS, (start + size) // LOCAL_BLOCKS)
            def _(step):
                local(slot, step * LOCAL_BLOCKS, last)

        for piece, (start, size) in enumerate(link_pieces[slot]):
            for link in range(CORE):
                copy = exchange(link, slot, piece)
                copy.wait_recv()
                copy.wait_send()

                @pl.loop(start, start + size)
                def _(block):
                    mix(link, slot, block, last)

            if not last:
                send_links(slot + 1, start, start + size)

    total = high_sum[HI_BITS]
    sublane = lax.broadcasted_iota(jnp.int32, (8, LANES), 0)
    lane = lax.broadcasted_iota(jnp.int32, (8, LANES), 1)
    signed = [total * (1 - 2 * own_bit).astype(jnp.float32) for own_bit in own_bits]
    signed += [high_sum[bit_pos] for bit_pos in range(HI_BITS)]
    low = [low_sum[8 * pos:8 * pos + 8, :] for pos in range(HALF // 8)]
    for bit_pos in range(ROW_BITS - 3):
        mask = 2 ** (ROW_BITS - 4 - bit_pos)
        signed.append(functools.reduce(jnp.add, [-part if pos & mask else part for pos, part in enumerate(low)]))
    signed += [jnp.where((sublane & (4 >> bit_pos)) != 0, -total, total) for bit_pos in range(3)]
    signed += [jnp.where((lane & (64 >> bit_pos)) != 0, -total, total) for bit_pos in range(LANE_BITS)]
    rows = [jnp.sum(part, axis=0, keepdims=True) for part in signed]
    table = jnp.concatenate(rows + [jnp.zeros((LANES - len(rows), LANES), jnp.float32)], axis=0)
    part = lax.dot_general(jnp.ones((8, LANES), jnp.float32), table, (((1,), (1,)), ((), ())), precision=HIGHEST, preferred_element_type=jnp.float32)
    part_ref[...] = part

    def share(offset):
        return pltpu.make_async_remote_copy(
            src_ref=part_ref, dst_ref=parts_ref.at[me], send_sem=part_send.at[offset], recv_sem=part_recv.at[me],
            device_id=((me + offset) % group_size,), device_id_type=MESH)

    def shared(offset):
        source = (me + group_size - offset) % group_size
        return pltpu.make_async_remote_copy(
            src_ref=part_ref, dst_ref=parts_ref.at[source], send_sem=part_send.at[offset], recv_sem=part_recv.at[source],
            device_id=((me + offset) % group_size,), device_id_type=MESH)

    for offset in range(1, group_size):
        share(offset).start()
    parts_ref[me] = part
    for offset in range(1, group_size):
        shared(offset).wait_recv()
    for offset in range(1, group_size):
        share(offset).wait_send()


def flush_kernel(scale, state_ref, parts_ref, out_ref, z_hbm, z_ref, sem, z_sem):
    size = BLOCKS // FLUSH_PIECES
    copies = []
    for quarter in range(QUARTERS):
        for piece in range(FLUSH_PIECES):
            span = pl.ds(piece * size, size)
            copies.append(pltpu.make_async_copy(state_ref.at[quarter, span], out_ref.at[quarter, span], sem.at[quarter, piece]))
    for copy in copies:
        copy.start()
    total = functools.reduce(jnp.add, [parts_ref[pos] for pos in range(parts_ref.shape[0])])
    z_ref[...] = total[0:1, :z_ref.shape[1]] * scale
    copies.append(pltpu.make_async_copy(z_ref, z_hbm, z_sem))
    copies[-1].start()
    for copy in copies:
        copy.wait()


def solution(mesh):
    group_size = mesh.shape['q']

    def local_layer(state_local, unitaries, cz_pairs):
        num_qubits = unitaries.shape[1]
        local_size = state_local.shape[1]
        row_count = local_size // LANES
        shape = (QUARTERS, BLOCKS, BLOCK_ROWS, LANES)
        grid = state_local.reshape(2, row_count, LANES).transpose(1, 0, 2).reshape(shape)
        state, parts = pl.pallas_call(
            functools.partial(kernel, group_size),
            out_shape=(pltpu.VMEM(shape, jnp.float32), pltpu.VMEM((group_size, 8, LANES), jnp.float32)),
            in_specs=[pl.BlockSpec(memory_space=pl.ANY)] * 3,
            out_specs=(pl.BlockSpec(memory_space=pltpu.VMEM), pl.BlockSpec(memory_space=pltpu.VMEM)),
            scratch_shapes=[
                pltpu.VMEM((TOP_BITS, 2, BLOCKS, BLOCK_ROWS, LANES), jnp.float32),
                pltpu.VMEM((2 * LANES, 2 * LANES), jnp.float32),
                pltpu.VMEM((BLOCK_ROWS, BLOCK_ROWS), jnp.float32),
                pltpu.VMEM((HALF, LANES), jnp.float32),
                pltpu.VMEM((HI_BITS + 1, 8, LANES), jnp.float32),
                pltpu.VMEM((8, LANES), jnp.float32),
                pltpu.SMEM((2, 2, 2, num_qubits), jnp.float32),
                pltpu.SMEM((2, cz_pairs.shape[0]), jnp.int32),
                pltpu.SMEM((cz_pairs.shape[0],), jnp.int32),
                pltpu.SemaphoreType.DMA((2,)),
                pltpu.SemaphoreType.REGULAR((TOP_BITS,)),
                pltpu.SemaphoreType.DMA((len(LOAD_SPANS),)),
                pltpu.SemaphoreType.DMA((TOP_BITS, 2, MAX_PIECES)),
                pltpu.SemaphoreType.DMA((TOP_BITS, 2, MAX_PIECES)),
                pltpu.SemaphoreType.DMA((group_size,)),
                pltpu.SemaphoreType.DMA((group_size,)),
            ],
            compiler_params=pltpu.CompilerParams(collective_id=0, has_side_effects=True, vmem_limit_bytes=44 * 1024 * 1024),
        )(grid, unitaries.transpose(0, 2, 3, 1), cz_pairs.T)
        state, z_expect = pl.pallas_call(
            functools.partial(flush_kernel, 1.0 / 2 ** num_qubits),
            out_shape=(jax.ShapeDtypeStruct(shape, jnp.float32), jax.ShapeDtypeStruct((1, num_qubits), jnp.float32)),
            in_specs=[pl.BlockSpec(memory_space=pltpu.VMEM)] * 2,
            out_specs=(pl.BlockSpec(memory_space=pl.ANY), pl.BlockSpec(memory_space=pl.ANY)),
            scratch_shapes=[pltpu.VMEM((1, num_qubits), jnp.float32), pltpu.SemaphoreType.DMA((QUARTERS, FLUSH_PIECES)), pltpu.SemaphoreType.DMA],
            compiler_params=pltpu.CompilerParams(vmem_limit_bytes=2 ** 20),
        )(pltpu.with_memory_space_constraint(state, pltpu.VMEM), pltpu.with_memory_space_constraint(parts, pltpu.VMEM))
        state = state.reshape(row_count, 2, LANES).transpose(1, 0, 2).reshape(2, local_size)
        return state, z_expect.reshape(num_qubits)

    return jax.shard_map(local_layer, mesh=mesh, in_specs=(P(None, 'q'), P(), P()), out_specs=(P(None, 'q'), P()), check_vma=False)
```

```python
import functools
import jax
import jax.numpy as jnp
from jax import lax
from jax.experimental import pallas as pl
from jax.experimental.pallas import tpu as pltpu
from jax.sharding import PartitionSpec as P

MESH = pl.DeviceIdType.MESH
LANES = 128
LANE_BITS = 7
ROW_BITS = 7
MID_BITS = 5
QUARTERS = 4
BLOCKS = 2 ** MID_BITS
BLOCK_ROWS = 2 * 2 ** ROW_BITS
HALF = BLOCK_ROWS // 2
LOCAL_BLOCKS = 2
LOAD_SPANS = (1, 6, 9, 16)
LINK_SPANS = ((1, 6, 9, 16), (16, 16), (16, 16), (16, 10, 3))
SWAP_BLOCKS = (29, 30, 31)
CORE_SPANS = (8, 8, 8, 8)
MAX_PIECES = 4
FLUSH_PIECES = 1
TOP_BITS = 4
CORE = 3
HI_BITS = 2 + MID_BITS
HIGHEST = lax.Precision.HIGHEST


def apply_coefs(coef_a, coef_b, first, second):
    out_re = coef_a[0] * first[0] - coef_a[1] * first[1] + coef_b[0] * second[0] - coef_b[1] * second[1]
    out_im = coef_a[0] * first[1] + coef_a[1] * first[0] + coef_b[0] * second[1] + coef_b[1] * second[0]
    return out_re, out_im


def gate_coefs(gates_ref, qubit):
    return [[(gates_ref[0, row, col, qubit], gates_ref[1, row, col, qubit]) for col in range(2)] for row in range(2)]


def pieces_of(spans):
    starts = [sum(spans[:pos]) for pos in range(len(spans))]
    return list(zip(starts, spans))


def butterfly(values, gates):
    size = len(values)
    for gate_pos, gate in enumerate(gates):
        stride = size >> (gate_pos + 1)
        values = list(values)
        for pos in range(size):
            if pos & stride:
                continue
            zero_half, one_half = values[pos], values[pos + stride]
            values[pos] = apply_coefs(gate[0][0], gate[0][1], zero_half, one_half)
            values[pos + stride] = apply_coefs(gate[1][0], gate[1][1], zero_half, one_half)
    return values


def load_rows(ref, row, rows):
    return ref[pl.ds(2 * row, rows, stride=2), :], ref[pl.ds(2 * row + 1, rows, stride=2), :]


def store_rows(ref, row, rows, value):
    ref[pl.ds(2 * row, rows, stride=2), :] = value[0]
    ref[pl.ds(2 * row + 1, rows, stride=2), :] = value[1]


def gate_blocks(refs, gates, rows):
    @pl.loop(0, HALF // rows)
    def _(group):
        row = pl.multiple_of(group * rows, rows)
        values = butterfly([load_rows(ref, row, rows) for ref in refs], gates)
        for ref, value in zip(refs, values):
            store_rows(ref, row, rows, value)


def build_matrix(mat_ref, gates_ref, first_qubit, num_bits, transposed):
    size = 2 ** num_bits
    out_index = lax.broadcasted_iota(jnp.int32, (size, size), 1 if transposed else 0)
    in_index = lax.broadcasted_iota(jnp.int32, (size, size), 0 if transposed else 1)
    prod_re = jnp.ones((size, size), jnp.float32)
    prod_im = jnp.zeros((size, size), jnp.float32)
    for bit_pos in range(num_bits):
        gate = gate_coefs(gates_ref, first_qubit + bit_pos)
        mask = 2 ** (num_bits - 1 - bit_pos)
        out_one = (out_index & mask) != 0
        in_one = (in_index & mask) != 0
        fac_re, fac_im = [jnp.where(out_one, jnp.where(in_one, gate[1][1][part], gate[1][0][part]), jnp.where(in_one, gate[0][1][part], gate[0][0][part])) for part in range(2)]
        prod_re, prod_im = prod_re * fac_re - prod_im * fac_im, prod_re * fac_im + prod_im * fac_re
    mat_ref[0:size, 0:size] = prod_re
    mat_ref[size:, size:] = prod_re
    mat_ref[0:size, size:] = prod_im if transposed else -prod_im
    mat_ref[size:, 0:size] = -prod_im if transposed else prod_im


def kernel(group_size, x_ref, gates_hbm, pairs_hbm, out_ref, parts_ref, recv_ref, lane_mat, row_mat, back_ref, low_sum, high_sum, sent_sum, part_ref,
           gates_ref, pairs_ref, mask_ref, small_sem, ready_sem, swap_sem, load_sem, send_sem, recv_sem, part_send, part_recv):
    num_qubits = gates_hbm.shape[3]
    num_pairs = pairs_hbm.shape[1]
    me = lax.axis_index('q')
    strides = [group_size >> (link + 1) for link in range(TOP_BITS)]
    own_bits = [(me // stride) % 2 for stride in strides]
    partners = [me + stride * (1 - 2 * own_bit) for stride, own_bit in zip(strides, own_bits)]

    load_pieces = pieces_of(LOAD_SPANS)
    link_pieces = [pieces_of(spans) for spans in LINK_SPANS]
    core_pieces = pieces_of(CORE_SPANS)

    def load(piece):
        span = pl.ds(*load_pieces[piece])
        return pltpu.make_async_copy(x_ref.at[:, span], out_ref.at[:, span], load_sem.at[piece])

    def exchange(link, slot, piece):
        span = pl.ds(*(core_pieces if link == CORE else link_pieces[slot])[piece])
        return pltpu.make_async_remote_copy(
            src_ref=out_ref.at[(slot + link) % 4, span], dst_ref=recv_ref.at[link, slot % 2, span],
            send_sem=send_sem.at[link, slot % 2, piece], recv_sem=recv_sem.at[link, slot % 2, piece],
            device_id=(partners[link],), device_id_type=MESH)

    def half_rows(bit):
        return pl.ds(pl.multiple_of(bit * HALF, HALF), HALF)

    def swap_out(link, swap):
        quarter, block, rows = (QUARTERS - 1 + link) % 4, SWAP_BLOCKS[swap], half_rows(1 - own_bits[link])
        return pltpu.make_async_remote_copy(
            src_ref=out_ref.at[quarter, block, rows], dst_ref=recv_ref.at[link, 1, block, rows],
            send_sem=swap_sem.at[0, link, swap], recv_sem=swap_sem.at[1, link, swap], device_id=(partners[link],), device_id_type=MESH)

    def swap_back(link, swap):
        return pltpu.make_async_remote_copy(
            src_ref=recv_ref.at[link, 1, SWAP_BLOCKS[swap], half_rows(own_bits[link])], dst_ref=back_ref.at[link, swap],
            send_sem=swap_sem.at[2, link, swap], recv_sem=swap_sem.at[3, link, swap], device_id=(partners[link],), device_id_type=MESH)

    def send_links(slot, done_from, done_to):
        for piece, (start, size) in enumerate(link_pieces[slot]):
            if done_from < start + size <= done_to:
                for link in range(CORE):
                    exchange(link, slot, piece).start()
        if slot == QUARTERS - 1:
            for swap, block in enumerate(SWAP_BLOCKS):
                if done_from <= block < done_to:
                    for link in range(CORE):
                        swap_out(link, swap).start()

    barrier = pltpu.get_barrier_semaphore()
    for partner in partners:
        pl.semaphore_signal(barrier, inc=1, device_id=(partner,), device_id_type=MESH)
    small = [pltpu.make_async_copy(gates_hbm, gates_ref, small_sem.at[0]), pltpu.make_async_copy(pairs_hbm, pairs_ref, small_sem.at[1])]
    load(0).start()
    for copy in small:
        copy.start()
    for piece in range(1, len(load_pieces)):
        load(piece).start()
    for copy in small:
        copy.wait()

    quarter_gates = [gate_coefs(gates_ref, TOP_BITS), gate_coefs(gates_ref, TOP_BITS + 1)]

    for piece, (start, size) in enumerate(load_pieces):
        load(piece).wait()

        @pl.loop(start, start + size)
        def _(block):
            gate_blocks([out_ref.at[quarter, block] for quarter in range(QUARTERS)], quarter_gates, 16)

        if piece == 0:
            pl.semaphore_wait(barrier, TOP_BITS)
        send_links(0, start, start + size)

    def mid_gates(quarter):
        first = TOP_BITS + 2
        gates = [gate_coefs(gates_ref, first + bit_pos) for bit_pos in range(MID_BITS)]

        @pl.loop(0, BLOCKS // 8)
        def _(low):
            gate_blocks([out_ref.at[quarter, pos * (BLOCKS // 8) + low] for pos in range(8)], gates[:3], 8)

        @pl.loop(0, BLOCKS // 4)
        def _(high):
            gate_blocks([out_ref.at[quarter, high * 4 + pos] for pos in range(4)], gates[3:], 16)

    def finish(target_ref, device, quarter, block, row, rows, value):
        first_row = ((device * QUARTERS + quarter) * BLOCKS + block) * HALF + row
        index = first_row * LANES + lax.broadcasted_iota(jnp.int32, (rows, LANES), 0) * LANES + lax.broadcasted_iota(jnp.int32, (rows, LANES), 1)
        odd = None
        for pair_pos in range(num_pairs):
            mask = mask_ref[pair_pos]
            hit = (index & mask) == mask
            odd = hit if odd is None else jnp.logical_xor(odd, hit)
        sign = jnp.where(odd, -1.0, 1.0)
        value = (value[0] * sign, value[1] * sign)
        store_rows(target_ref, row, rows, value)
        density = value[0] * value[0] + value[1] * value[1]
        low_sum[pl.ds(row, rows), :] += density
        return jnp.sum(density.reshape(rows // 8, 8, LANES), axis=0)

    def add_high(quarter, block, total):
        position = quarter * BLOCKS + block
        for bit_pos in range(HI_BITS):
            bit = (position // 2 ** (HI_BITS - 1 - bit_pos)) % 2
            high_sum[bit_pos] += total * jnp.asarray(1 - 2 * bit, jnp.float32)
        high_sum[HI_BITS] += total

    def mix(link, slot, block, last):
        quarter = (slot + link) % 4
        own_bit = own_bits[link]
        coef_self = [gates_ref[part, own_bit, own_bit, link] for part in range(2)]
        coef_other = [gates_ref[part, own_bit, 1 - own_bit, link] for part in range(2)]
        rows = 32
        own_ref = out_ref.at[quarter, block]
        other_ref = recv_ref.at[link, slot % 2, block]

        def body(group, total):
            row = pl.multiple_of(group * rows, rows)
            value = apply_coefs(coef_self, coef_other, load_rows(own_ref, row, rows), load_rows(other_ref, row, rows))
            if last:
                return total + finish(own_ref, me, quarter, block, row, rows, value)
            store_rows(own_ref, row, rows, value)
            return total

        total = lax.fori_loop(0, HALF // rows, body, jnp.zeros((8, LANES), jnp.float32))
        if last:
            add_high(quarter, block, total)

    def mix_swap(link, swap):
        quarter, block = (QUARTERS - 1 + link) % 4, SWAP_BLOCKS[swap]
        own_bit = own_bits[link]
        home, away = [[[gates_ref[part, row_bit, col_bit, link] for part in range(2)] for col_bit in (own_bit, 1 - own_bit)] for row_bit in (own_bit, 1 - own_bit)]
        rows = 32
        own_ref = out_ref.at[quarter, block]
        other_ref = recv_ref.at[link, 1, block]

        def body(group, totals):
            row = pl.multiple_of(own_bit * (HALF // 2) + group * rows, rows)
            own, other = load_rows(own_ref, row, rows), load_rows(other_ref, row, rows)
            kept = finish(own_ref, me, quarter, block, row, rows, apply_coefs(home[0], home[1], own, other))
            sent = finish(other_ref, partners[link], quarter, block, row, rows, apply_coefs(away[0], away[1], own, other))
            return totals[0] + kept, totals[1] + sent

        zero = jnp.zeros((8, LANES), jnp.float32)
        kept, sent = lax.fori_loop(0, HALF // 2 // rows, body, (zero, zero))
        add_high(quarter, block, kept + sent)
        sent_sum[link] += sent

    def local(slot, first_block, last):
        quarter = (slot + CORE) % 4
        blocks = [first_block + pos for pos in range(LOCAL_BLOCKS)]
        for block in blocks:
            mix(CORE, slot, block, False)
        refs = [out_ref.at[quarter, block] for block in blocks]
        parts = [load_rows(ref, 0, HALF) for ref in refs]
        rows = jnp.concatenate([jnp.concatenate(part, axis=1) for part in parts], axis=0)
        mixed = jnp.dot(rows, lane_mat[...], precision=HIGHEST, preferred_element_type=jnp.float32)
        columns = jnp.concatenate([
            jnp.concatenate([mixed[pos * HALF:(pos + 1) * HALF, :LANES], mixed[pos * HALF:(pos + 1) * HALF, LANES:]], axis=0)
            for pos in range(LOCAL_BLOCKS)], axis=1)
        done = jnp.dot(row_mat[...], columns, precision=HIGHEST, preferred_element_type=jnp.float32)
        for pos, ref in enumerate(refs):
            piece = done[:, pos * LANES:(pos + 1) * LANES]
            store_rows(ref, 0, HALF, (piece[:HALF], piece[HALF:]))
        if last:
            group_rows = 32
            for block in blocks:
                def body(group, total):
                    row = pl.multiple_of(group * group_rows, group_rows)
                    return total + finish(out_ref.at[quarter, block], me, quarter, block, row, group_rows, load_rows(out_ref.at[quarter, block], row, group_rows))

                total = lax.fori_loop(0, HALF // group_rows, body, jnp.zeros((8, LANES), jnp.float32))
                add_high(quarter, block, total)

    for pair_pos in range(num_pairs):
        mask_ref[pair_pos] = (1 << (num_qubits - 1 - pairs_ref[0, pair_pos])) | (1 << (num_qubits - 1 - pairs_ref[1, pair_pos]))
    low_sum[...] = jnp.zeros_like(low_sum)
    high_sum[...] = jnp.zeros_like(high_sum)
    sent_sum[...] = jnp.zeros_like(sent_sum)
    for link, partner in enumerate(partners):
        pl.semaphore_signal(ready_sem.at[link], inc=1, device_id=(partner,), device_id_type=MESH)
        pl.semaphore_wait(ready_sem.at[link], 1)
    build_matrix(lane_mat, gates_ref, num_qubits - LANE_BITS, LANE_BITS, True)
    build_matrix(row_mat, gates_ref, num_qubits - LANE_BITS - ROW_BITS, ROW_BITS, False)
    for slot in range(QUARTERS):
        last = slot == QUARTERS - 1
        mid_gates((slot + CORE) % 4)
        for piece in range(len(core_pieces)):
            exchange(CORE, slot, piece).start()
        for piece, (start, size) in enumerate(core_pieces):
            copy = exchange(CORE, slot, piece)
            copy.wait_recv()
            copy.wait_send()

            @pl.loop(start // LOCAL_BLOCKS, (start + size) // LOCAL_BLOCKS)
            def _(step):
                local(slot, step * LOCAL_BLOCKS, last)

        for piece, (start, size) in enumerate(link_pieces[slot]):
            for link in range(CORE):
                copy = exchange(link, slot, piece)
                copy.wait_recv()
                copy.wait_send()

                @pl.loop(start, start + size)
                def _(block):
                    mix(link, slot, block, last)

            if not last:
                send_links(slot + 1, start, start + size)

    for swap in range(len(SWAP_BLOCKS)):
        for link in range(CORE):
            copy = swap_out(link, swap)
            copy.wait_recv()
            copy.wait_send()
            mix_swap(link, swap)
        if swap < len(SWAP_BLOCKS) - 1:
            for link in range(CORE):
                swap_back(link, swap).start()

    total = high_sum[HI_BITS]
    sublane = lax.broadcasted_iota(jnp.int32, (8, LANES), 0)
    lane = lax.broadcasted_iota(jnp.int32, (8, LANES), 1)
    signed = [(total - 2.0 * sent_sum[link]) * (1 - 2 * own_bit).astype(jnp.float32) for link, own_bit in enumerate(own_bits)]
    signed += [high_sum[bit_pos] for bit_pos in range(HI_BITS)]
    low = [low_sum[8 * pos:8 * pos + 8, :] for pos in range(HALF // 8)]
    for bit_pos in range(ROW_BITS - 3):
        mask = 2 ** (ROW_BITS - 4 - bit_pos)
        signed.append(functools.reduce(jnp.add, [-part if pos & mask else part for pos, part in enumerate(low)]))
    signed += [jnp.where((sublane & (4 >> bit_pos)) != 0, -total, total) for bit_pos in range(3)]
    signed += [jnp.where((lane & (64 >> bit_pos)) != 0, -total, total) for bit_pos in range(LANE_BITS)]
    rows = [jnp.sum(part, axis=0, keepdims=True) for part in signed]
    table = jnp.concatenate(rows + [jnp.zeros((LANES - len(rows), LANES), jnp.float32)], axis=0)
    part = lax.dot_general(jnp.ones((8, LANES), jnp.float32), table, (((1,), (1,)), ((), ())), precision=HIGHEST, preferred_element_type=jnp.float32)
    part_ref[...] = part

    def share(offset):
        return pltpu.make_async_remote_copy(
            src_ref=part_ref, dst_ref=parts_ref.at[me], send_sem=part_send.at[offset], recv_sem=part_recv.at[me],
            device_id=((me + offset) % group_size,), device_id_type=MESH)

    def shared(offset):
        source = (me + group_size - offset) % group_size
        return pltpu.make_async_remote_copy(
            src_ref=part_ref, dst_ref=parts_ref.at[source], send_sem=part_send.at[offset], recv_sem=part_recv.at[source],
            device_id=((me + offset) % group_size,), device_id_type=MESH)

    for offset in range(1, group_size):
        share(offset).start()
    for link in range(CORE):
        swap_back(link, len(SWAP_BLOCKS) - 1).start()
    parts_ref[me] = part
    for swap in range(len(SWAP_BLOCKS)):
        for link in range(CORE):
            copy = swap_back(link, swap)
            copy.wait_recv()
            out_ref[(QUARTERS - 1 + link) % 4, SWAP_BLOCKS[swap], half_rows(1 - own_bits[link]), :] = back_ref[link, swap]
            copy.wait_send()
    for offset in range(1, group_size):
        shared(offset).wait_recv()
    for offset in range(1, group_size):
        share(offset).wait_send()


def flush_kernel(scale, state_ref, parts_ref, out_ref, z_hbm, z_ref, sem, z_sem):
    size = BLOCKS // FLUSH_PIECES
    copies = []
    for quarter in range(QUARTERS):
        for piece in range(FLUSH_PIECES):
            span = pl.ds(piece * size, size)
            copies.append(pltpu.make_async_copy(state_ref.at[quarter, span], out_ref.at[quarter, span], sem.at[quarter, piece]))
    for copy in copies:
        copy.start()
    total = functools.reduce(jnp.add, [parts_ref[pos] for pos in range(parts_ref.shape[0])])
    z_ref[...] = total[0:1, :z_ref.shape[1]] * scale
    copies.append(pltpu.make_async_copy(z_ref, z_hbm, z_sem))
    copies[-1].start()
    for copy in copies:
        copy.wait()


def solution(mesh):
    group_size = mesh.shape['q']

    def local_layer(state_local, unitaries, cz_pairs):
        num_qubits = unitaries.shape[1]
        local_size = state_local.shape[1]
        row_count = local_size // LANES
        shape = (QUARTERS, BLOCKS, BLOCK_ROWS, LANES)
        grid = state_local.reshape(2, row_count, LANES).transpose(1, 0, 2).reshape(shape)
        state, parts = pl.pallas_call(
            functools.partial(kernel, group_size),
            out_shape=(pltpu.VMEM(shape, jnp.float32), pltpu.VMEM((group_size, 8, LANES), jnp.float32)),
            in_specs=[pl.BlockSpec(memory_space=pl.ANY)] * 3,
            out_specs=(pl.BlockSpec(memory_space=pltpu.VMEM), pl.BlockSpec(memory_space=pltpu.VMEM)),
            scratch_shapes=[
                pltpu.VMEM((TOP_BITS, 2, BLOCKS, BLOCK_ROWS, LANES), jnp.float32),
                pltpu.VMEM((2 * LANES, 2 * LANES), jnp.float32),
                pltpu.VMEM((BLOCK_ROWS, BLOCK_ROWS), jnp.float32),
                pltpu.VMEM((CORE, len(SWAP_BLOCKS), HALF, LANES), jnp.float32),
                pltpu.VMEM((HALF, LANES), jnp.float32),
                pltpu.VMEM((HI_BITS + 1, 8, LANES), jnp.float32),
                pltpu.VMEM((TOP_BITS, 8, LANES), jnp.float32),
                pltpu.VMEM((8, LANES), jnp.float32),
                pltpu.SMEM((2, 2, 2, num_qubits), jnp.float32),
                pltpu.SMEM((2, cz_pairs.shape[0]), jnp.int32),
                pltpu.SMEM((cz_pairs.shape[0],), jnp.int32),
                pltpu.SemaphoreType.DMA((2,)),
                pltpu.SemaphoreType.REGULAR((TOP_BITS,)),
                pltpu.SemaphoreType.DMA((4, CORE, len(SWAP_BLOCKS))),
                pltpu.SemaphoreType.DMA((len(LOAD_SPANS),)),
                pltpu.SemaphoreType.DMA((TOP_BITS, 2, MAX_PIECES)),
                pltpu.SemaphoreType.DMA((TOP_BITS, 2, MAX_PIECES)),
                pltpu.SemaphoreType.DMA((group_size,)),
                pltpu.SemaphoreType.DMA((group_size,)),
            ],
            compiler_params=pltpu.CompilerParams(collective_id=0, has_side_effects=True, vmem_limit_bytes=44 * 1024 * 1024),
        )(grid, unitaries.transpose(0, 2, 3, 1), cz_pairs.T)
        state, z_expect = pl.pallas_call(
            functools.partial(flush_kernel, 1.0 / 2 ** num_qubits),
            out_shape=(jax.ShapeDtypeStruct(shape, jnp.float32), jax.ShapeDtypeStruct((1, num_qubits), jnp.float32)),
            in_specs=[pl.BlockSpec(memory_space=pltpu.VMEM)] * 2,
            out_specs=(pl.BlockSpec(memory_space=pl.ANY), pl.BlockSpec(memory_space=pl.ANY)),
            scratch_shapes=[pltpu.VMEM((1, num_qubits), jnp.float32), pltpu.SemaphoreType.DMA((QUARTERS, FLUSH_PIECES)), pltpu.SemaphoreType.DMA],
            compiler_params=pltpu.CompilerParams(vmem_limit_bytes=2 ** 20),
        )(pltpu.with_memory_space_constraint(state, pltpu.VMEM), pltpu.with_memory_space_constraint(parts, pltpu.VMEM))
        state = state.reshape(row_count, 2, LANES).transpose(1, 0, 2).reshape(2, local_size)
        return state, z_expect.reshape(num_qubits)

    return jax.shard_map(local_layer, mesh=mesh, in_specs=(P(None, 'q'), P(), P()), out_specs=(P(None, 'q'), P()), check_vma=False)
```

```python
import functools
import jax
import jax.numpy as jnp
from jax import lax
from jax.experimental import pallas as pl
from jax.experimental.pallas import tpu as pltpu
from jax.sharding import PartitionSpec as P

MESH = pl.DeviceIdType.MESH
LANES = 128
LANE_BITS = 7
ROW_BITS = 7
MID_BITS = 5
QUARTERS = 4
BLOCKS = 2 ** MID_BITS
BLOCK_ROWS = 2 * 2 ** ROW_BITS
HALF = BLOCK_ROWS // 2
LOCAL_BLOCKS = 2
LOAD_SPANS = (1, 6, 9, 16)
LINK_SPANS = ((1, 6, 9, 16), (16, 16), (16, 16), (16, 10, 3))
SWAP_BLOCKS = (29, 30, 31)
CORE_SPANS = (8, 8, 8, 8)
MAX_PIECES = 4
FLUSH_PIECES = 1
TOP_BITS = 4
CORE = 3
HI_BITS = 2 + MID_BITS
HIGHEST = lax.Precision.HIGHEST


def apply_coefs(coef_a, coef_b, first, second):
    out_re = coef_a[0] * first[0] - coef_a[1] * first[1] + coef_b[0] * second[0] - coef_b[1] * second[1]
    out_im = coef_a[0] * first[1] + coef_a[1] * first[0] + coef_b[0] * second[1] + coef_b[1] * second[0]
    return out_re, out_im


def gate_coefs(gates_ref, qubit):
    return [[(gates_ref[0, row, col, qubit], gates_ref[1, row, col, qubit]) for col in range(2)] for row in range(2)]


def pieces_of(spans):
    starts = [sum(spans[:pos]) for pos in range(len(spans))]
    return list(zip(starts, spans))


def butterfly(values, gates):
    size = len(values)
    for gate_pos, gate in enumerate(gates):
        stride = size >> (gate_pos + 1)
        values = list(values)
        for pos in range(size):
            if pos & stride:
                continue
            zero_half, one_half = values[pos], values[pos + stride]
            values[pos] = apply_coefs(gate[0][0], gate[0][1], zero_half, one_half)
            values[pos + stride] = apply_coefs(gate[1][0], gate[1][1], zero_half, one_half)
    return values


def load_rows(ref, row, rows):
    return ref[pl.ds(2 * row, rows, stride=2), :], ref[pl.ds(2 * row + 1, rows, stride=2), :]


def store_rows(ref, row, rows, value):
    ref[pl.ds(2 * row, rows, stride=2), :] = value[0]
    ref[pl.ds(2 * row + 1, rows, stride=2), :] = value[1]


def gate_blocks(refs, gates, rows):
    @pl.loop(0, HALF // rows)
    def _(group):
        row = pl.multiple_of(group * rows, rows)
        values = butterfly([load_rows(ref, row, rows) for ref in refs], gates)
        for ref, value in zip(refs, values):
            store_rows(ref, row, rows, value)


def build_matrix(mat_ref, gates_ref, first_qubit, num_bits, transposed):
    size = 2 ** num_bits
    out_index = lax.broadcasted_iota(jnp.int32, (size, size), 1 if transposed else 0)
    in_index = lax.broadcasted_iota(jnp.int32, (size, size), 0 if transposed else 1)
    prod_re = jnp.ones((size, size), jnp.float32)
    prod_im = jnp.zeros((size, size), jnp.float32)
    for bit_pos in range(num_bits):
        gate = gate_coefs(gates_ref, first_qubit + bit_pos)
        mask = 2 ** (num_bits - 1 - bit_pos)
        out_one = (out_index & mask) != 0
        in_one = (in_index & mask) != 0
        fac_re, fac_im = [jnp.where(out_one, jnp.where(in_one, gate[1][1][part], gate[1][0][part]), jnp.where(in_one, gate[0][1][part], gate[0][0][part])) for part in range(2)]
        prod_re, prod_im = prod_re * fac_re - prod_im * fac_im, prod_re * fac_im + prod_im * fac_re
    mat_ref[0:size, 0:size] = prod_re
    mat_ref[size:, size:] = prod_re
    mat_ref[0:size, size:] = prod_im if transposed else -prod_im
    mat_ref[size:, 0:size] = -prod_im if transposed else prod_im


def kernel(group_size, x_ref, gates_hbm, pairs_hbm, out_ref, parts_ref, recv_ref, lane_mat, row_mat, back_ref, low_sum, high_sum, sent_sum, part_ref,
           gates_ref, pairs_ref, mask_ref, small_sem, ready_sem, swap_sem, load_sem, send_sem, recv_sem, part_send, part_recv):
    num_qubits = gates_hbm.shape[3]
    num_pairs = pairs_hbm.shape[1]
    me = lax.axis_index('q')
    strides = [group_size >> (link + 1) for link in range(TOP_BITS)]
    own_bits = [(me // stride) % 2 for stride in strides]
    partners = [me + stride * (1 - 2 * own_bit) for stride, own_bit in zip(strides, own_bits)]

    load_pieces = pieces_of(LOAD_SPANS)
    link_pieces = [pieces_of(spans) for spans in LINK_SPANS]
    core_pieces = pieces_of(CORE_SPANS)

    def load(piece):
        span = pl.ds(*load_pieces[piece])
        return pltpu.make_async_copy(x_ref.at[:, span], out_ref.at[:, span], load_sem.at[piece])

    def exchange(link, slot, piece):
        span = pl.ds(*(core_pieces if link == CORE else link_pieces[slot])[piece])
        return pltpu.make_async_remote_copy(
            src_ref=out_ref.at[(slot + link) % 4, span], dst_ref=recv_ref.at[link, slot % 2, span],
            send_sem=send_sem.at[link, slot % 2, piece], recv_sem=recv_sem.at[link, slot % 2, piece],
            device_id=(partners[link],), device_id_type=MESH)

    def half_rows(bit):
        return pl.ds(pl.multiple_of(bit * HALF, HALF), HALF)

    def swap_out(link, swap):
        quarter, block, rows = (QUARTERS - 1 + link) % 4, SWAP_BLOCKS[swap], half_rows(1 - own_bits[link])
        return pltpu.make_async_remote_copy(
            src_ref=out_ref.at[quarter, block, rows], dst_ref=recv_ref.at[link, 1, block, rows],
            send_sem=swap_sem.at[0, link, swap], recv_sem=swap_sem.at[1, link, swap], device_id=(partners[link],), device_id_type=MESH)

    def swap_back(link, swap):
        return pltpu.make_async_remote_copy(
            src_ref=recv_ref.at[link, 1, SWAP_BLOCKS[swap], half_rows(own_bits[link])], dst_ref=back_ref.at[link, swap],
            send_sem=swap_sem.at[2, link, swap], recv_sem=swap_sem.at[3, link, swap], device_id=(partners[link],), device_id_type=MESH)

    def send_links(slot, done_from, done_to):
        for piece, (start, size) in enumerate(link_pieces[slot]):
            if done_from < start + size <= done_to:
                for link in range(CORE):
                    exchange(link, slot, piece).start()
        if slot == QUARTERS - 1:
            for swap, block in enumerate(SWAP_BLOCKS):
                if done_from <= block < done_to:
                    for link in range(CORE):
                        swap_out(link, swap).start()

    barrier = pltpu.get_barrier_semaphore()
    for partner in partners:
        pl.semaphore_signal(barrier, inc=1, device_id=(partner,), device_id_type=MESH)
    small = [pltpu.make_async_copy(gates_hbm, gates_ref, small_sem.at[0]), pltpu.make_async_copy(pairs_hbm, pairs_ref, small_sem.at[1])]
    load(0).start()
    for copy in small:
        copy.start()
    for piece in range(1, len(load_pieces)):
        load(piece).start()
    for copy in small:
        copy.wait()

    quarter_gates = [gate_coefs(gates_ref, TOP_BITS), gate_coefs(gates_ref, TOP_BITS + 1)]

    for piece, (start, size) in enumerate(load_pieces):
        load(piece).wait()

        @pl.loop(start, start + size)
        def _(block):
            gate_blocks([out_ref.at[quarter, block] for quarter in range(QUARTERS)], quarter_gates, 16)

        if piece == 0:
            pl.semaphore_wait(barrier, TOP_BITS)
        send_links(0, start, start + size)

    def mid_gates(quarter):
        first = TOP_BITS + 2
        gates = [gate_coefs(gates_ref, first + bit_pos) for bit_pos in range(MID_BITS)]

        @pl.loop(0, BLOCKS // 8)
        def _(low):
            gate_blocks([out_ref.at[quarter, pos * (BLOCKS // 8) + low] for pos in range(8)], gates[:3], 8)

        @pl.loop(0, BLOCKS // 4)
        def _(high):
            gate_blocks([out_ref.at[quarter, high * 4 + pos] for pos in range(4)], gates[3:], 16)

    def finish(target_ref, device, quarter, block, row, rows, value):
        first_row = ((device * QUARTERS + quarter) * BLOCKS + block) * HALF + row
        index = first_row * LANES + lax.broadcasted_iota(jnp.int32, (rows, LANES), 0) * LANES + lax.broadcasted_iota(jnp.int32, (rows, LANES), 1)
        odd = None
        for pair_pos in range(num_pairs):
            mask = mask_ref[pair_pos]
            hit = (index & mask) == mask
            odd = hit if odd is None else jnp.logical_xor(odd, hit)
        sign = jnp.where(odd, -1.0, 1.0)
        value = (value[0] * sign, value[1] * sign)
        store_rows(target_ref, row, rows, value)
        density = value[0] * value[0] + value[1] * value[1]
        low_sum[pl.ds(row, rows), :] += density
        return jnp.sum(density.reshape(rows // 8, 8, LANES), axis=0)

    def add_high(quarter, block, total):
        position = quarter * BLOCKS + block
        for bit_pos in range(HI_BITS):
            bit = (position // 2 ** (HI_BITS - 1 - bit_pos)) % 2
            high_sum[bit_pos] += total * jnp.asarray(1 - 2 * bit, jnp.float32)
        high_sum[HI_BITS] += total

    def mix(link, slot, block, last):
        quarter = (slot + link) % 4
        own_bit = own_bits[link]
        coef_self = [gates_ref[part, own_bit, own_bit, link] for part in range(2)]
        coef_other = [gates_ref[part, own_bit, 1 - own_bit, link] for part in range(2)]
        rows = 32
        own_ref = out_ref.at[quarter, block]
        other_ref = recv_ref.at[link, slot % 2, block]

        def body(group, total):
            row = pl.multiple_of(group * rows, rows)
            value = apply_coefs(coef_self, coef_other, load_rows(own_ref, row, rows), load_rows(other_ref, row, rows))
            if last:
                return total + finish(own_ref, me, quarter, block, row, rows, value)
            store_rows(own_ref, row, rows, value)
            return total

        total = lax.fori_loop(0, HALF // rows, body, jnp.zeros((8, LANES), jnp.float32))
        if last:
            add_high(quarter, block, total)

    def mix_swap(link, swap):
        quarter, block = (QUARTERS - 1 + link) % 4, SWAP_BLOCKS[swap]
        own_bit = own_bits[link]
        home, away = [[[gates_ref[part, row_bit, col_bit, link] for part in range(2)] for col_bit in (own_bit, 1 - own_bit)] for row_bit in (own_bit, 1 - own_bit)]
        rows = 32
        own_ref = out_ref.at[quarter, block]
        other_ref = recv_ref.at[link, 1, block]

        def body(group, totals):
            row = pl.multiple_of(own_bit * (HALF // 2) + group * rows, rows)
            own, other = load_rows(own_ref, row, rows), load_rows(other_ref, row, rows)
            kept = finish(own_ref, me, quarter, block, row, rows, apply_coefs(home[0], home[1], own, other))
            sent = finish(other_ref, partners[link], quarter, block, row, rows, apply_coefs(away[0], away[1], own, other))
            return totals[0] + kept, totals[1] + sent

        zero = jnp.zeros((8, LANES), jnp.float32)
        kept, sent = lax.fori_loop(0, HALF // 2 // rows, body, (zero, zero))
        add_high(quarter, block, kept + sent)
        sent_sum[link] += sent

    def local(slot, first_block, last):
        quarter = (slot + CORE) % 4
        blocks = [first_block + pos for pos in range(LOCAL_BLOCKS)]
        for block in blocks:
            mix(CORE, slot, block, False)
        refs = [out_ref.at[quarter, block] for block in blocks]
        parts = [load_rows(ref, 0, HALF) for ref in refs]
        rows = jnp.concatenate([jnp.concatenate(part, axis=1) for part in parts], axis=0)
        mixed = jnp.dot(rows, lane_mat[...], precision=HIGHEST, preferred_element_type=jnp.float32)
        columns = jnp.concatenate([
            jnp.concatenate([mixed[pos * HALF:(pos + 1) * HALF, :LANES], mixed[pos * HALF:(pos + 1) * HALF, LANES:]], axis=0)
            for pos in range(LOCAL_BLOCKS)], axis=1)
        done = jnp.dot(row_mat[...], columns, precision=HIGHEST, preferred_element_type=jnp.float32)
        for pos, ref in enumerate(refs):
            piece = done[:, pos * LANES:(pos + 1) * LANES]
            store_rows(ref, 0, HALF, (piece[:HALF], piece[HALF:]))
        if last:
            group_rows = 32
            for block in blocks:
                def body(group, total):
                    row = pl.multiple_of(group * group_rows, group_rows)
                    return total + finish(out_ref.at[quarter, block], me, quarter, block, row, group_rows, load_rows(out_ref.at[quarter, block], row, group_rows))

                total = lax.fori_loop(0, HALF // group_rows, body, jnp.zeros((8, LANES), jnp.float32))
                add_high(quarter, block, total)

    for pair_pos in range(num_pairs):
        mask_ref[pair_pos] = (1 << (num_qubits - 1 - pairs_ref[0, pair_pos])) | (1 << (num_qubits - 1 - pairs_ref[1, pair_pos]))
    low_sum[...] = jnp.zeros_like(low_sum)
    high_sum[...] = jnp.zeros_like(high_sum)
    sent_sum[...] = jnp.zeros_like(sent_sum)
    for link, partner in enumerate(partners):
        pl.semaphore_signal(ready_sem.at[link], inc=1, device_id=(partner,), device_id_type=MESH)
        pl.semaphore_wait(ready_sem.at[link], 1)
    build_matrix(lane_mat, gates_ref, num_qubits - LANE_BITS, LANE_BITS, True)
    build_matrix(row_mat, gates_ref, num_qubits - LANE_BITS - ROW_BITS, ROW_BITS, False)
    for slot in range(QUARTERS):
        last = slot == QUARTERS - 1
        mid_gates((slot + CORE) % 4)
        for piece in range(len(core_pieces)):
            exchange(CORE, slot, piece).start()
        for piece, (start, size) in enumerate(core_pieces):
            copy = exchange(CORE, slot, piece)
            copy.wait_recv()
            copy.wait_send()

            @pl.loop(start // LOCAL_BLOCKS, (start + size) // LOCAL_BLOCKS)
            def _(step):
                local(slot, step * LOCAL_BLOCKS, last)

        for piece, (start, size) in enumerate(link_pieces[slot]):
            for link in range(CORE):
                copy = exchange(link, slot, piece)
                copy.wait_recv()
                copy.wait_send()

                @pl.loop(start, start + size)
                def _(block):
                    mix(link, slot, block, last)

            if not last:
                send_links(slot + 1, start, start + size)

    for swap in range(len(SWAP_BLOCKS)):
        for link in range(CORE):
            copy = swap_out(link, swap)
            copy.wait_recv()
            copy.wait_send()
            mix_swap(link, swap)
        if swap < len(SWAP_BLOCKS) - 1:
            for link in range(CORE):
                swap_back(link, swap).start()

    total = high_sum[HI_BITS]
    sublane = lax.broadcasted_iota(jnp.int32, (8, LANES), 0)
    lane = lax.broadcasted_iota(jnp.int32, (8, LANES), 1)
    signed = [(total - 2.0 * sent_sum[link]) * (1 - 2 * own_bit).astype(jnp.float32) for link, own_bit in enumerate(own_bits)]
    signed += [high_sum[bit_pos] for bit_pos in range(HI_BITS)]
    low = [low_sum[8 * pos:8 * pos + 8, :] for pos in range(HALF // 8)]
    for bit_pos in range(ROW_BITS - 3):
        mask = 2 ** (ROW_BITS - 4 - bit_pos)
        signed.append(functools.reduce(jnp.add, [-part if pos & mask else part for pos, part in enumerate(low)]))
    signed += [jnp.where((sublane & (4 >> bit_pos)) != 0, -total, total) for bit_pos in range(3)]
    signed += [jnp.where((lane & (64 >> bit_pos)) != 0, -total, total) for bit_pos in range(LANE_BITS)]
    rows = [jnp.sum(part, axis=0, keepdims=True) for part in signed]
    table = jnp.concatenate(rows + [jnp.zeros((LANES - len(rows), LANES), jnp.float32)], axis=0)
    part = lax.dot_general(jnp.ones((8, LANES), jnp.float32), table, (((1,), (1,)), ((), ())), precision=HIGHEST, preferred_element_type=jnp.float32)
    part_ref[0] = part

    chips = group_size // 2
    pair = pltpu.make_async_remote_copy(
        src_ref=part_ref.at[0], dst_ref=part_ref.at[1], send_sem=part_send.at[0], recv_sem=part_recv.at[chips],
        device_id=(partners[CORE],), device_id_type=MESH)
    pair.start()
    pair.wait_recv()
    chip_part = part + part_ref[1]
    part_ref[2] = chip_part

    def share(offset, slot):
        return pltpu.make_async_remote_copy(
            src_ref=part_ref.at[2, pl.ds(0, 1)], dst_ref=parts_ref.at[slot, pl.ds(0, 1)], send_sem=part_send.at[offset], recv_sem=part_recv.at[slot],
            device_id=((me + 2 * offset) % group_size,), device_id_type=MESH)

    for offset in range(1, chips):
        share(offset, me // 2).start()
    for link in range(CORE):
        swap_back(link, len(SWAP_BLOCKS) - 1).start()
    parts_ref[me // 2] = chip_part
    pair.wait_send()
    for swap in range(len(SWAP_BLOCKS)):
        for link in range(CORE):
            copy = swap_back(link, swap)
            copy.wait_recv()
            out_ref[(QUARTERS - 1 + link) % 4, SWAP_BLOCKS[swap], half_rows(1 - own_bits[link]), :] = back_ref[link, swap]
            copy.wait_send()
    for offset in range(1, chips):
        share(offset, (me // 2 + chips - offset) % chips).wait_recv()
    for offset in range(1, chips):
        share(offset, me // 2).wait_send()


def flush_kernel(scale, state_ref, parts_ref, out_ref, z_hbm, z_ref, sem, z_sem):
    size = BLOCKS // FLUSH_PIECES
    copies = []
    for quarter in range(QUARTERS):
        for piece in range(FLUSH_PIECES):
            span = pl.ds(piece * size, size)
            copies.append(pltpu.make_async_copy(state_ref.at[quarter, span], out_ref.at[quarter, span], sem.at[quarter, piece]))
    for copy in copies:
        copy.start()
    total = functools.reduce(jnp.add, [parts_ref[pos, 0:1, :] for pos in range(parts_ref.shape[0])])
    z_ref[...] = total[:, :z_ref.shape[1]] * scale
    copies.append(pltpu.make_async_copy(z_ref, z_hbm, z_sem))
    copies[-1].start()
    for copy in copies:
        copy.wait()


def solution(mesh):
    group_size = mesh.shape['q']

    def local_layer(state_local, unitaries, cz_pairs):
        num_qubits = unitaries.shape[1]
        local_size = state_local.shape[1]
        row_count = local_size // LANES
        shape = (QUARTERS, BLOCKS, BLOCK_ROWS, LANES)
        grid = state_local.reshape(2, row_count, LANES).transpose(1, 0, 2).reshape(shape)
        state, parts = pl.pallas_call(
            functools.partial(kernel, group_size),
            out_shape=(pltpu.VMEM(shape, jnp.float32), pltpu.VMEM((group_size // 2, 8, LANES), jnp.float32)),
            in_specs=[pl.BlockSpec(memory_space=pl.ANY)] * 3,
            out_specs=(pl.BlockSpec(memory_space=pltpu.VMEM), pl.BlockSpec(memory_space=pltpu.VMEM)),
            scratch_shapes=[
                pltpu.VMEM((TOP_BITS, 2, BLOCKS, BLOCK_ROWS, LANES), jnp.float32),
                pltpu.VMEM((2 * LANES, 2 * LANES), jnp.float32),
                pltpu.VMEM((BLOCK_ROWS, BLOCK_ROWS), jnp.float32),
                pltpu.VMEM((CORE, len(SWAP_BLOCKS), HALF, LANES), jnp.float32),
                pltpu.VMEM((HALF, LANES), jnp.float32),
                pltpu.VMEM((HI_BITS + 1, 8, LANES), jnp.float32),
                pltpu.VMEM((TOP_BITS, 8, LANES), jnp.float32),
                pltpu.VMEM((3, 8, LANES), jnp.float32),
                pltpu.SMEM((2, 2, 2, num_qubits), jnp.float32),
                pltpu.SMEM((2, cz_pairs.shape[0]), jnp.int32),
                pltpu.SMEM((cz_pairs.shape[0],), jnp.int32),
                pltpu.SemaphoreType.DMA((2,)),
                pltpu.SemaphoreType.REGULAR((TOP_BITS,)),
                pltpu.SemaphoreType.DMA((4, CORE, len(SWAP_BLOCKS))),
                pltpu.SemaphoreType.DMA((len(LOAD_SPANS),)),
                pltpu.SemaphoreType.DMA((TOP_BITS, 2, MAX_PIECES)),
                pltpu.SemaphoreType.DMA((TOP_BITS, 2, MAX_PIECES)),
                pltpu.SemaphoreType.DMA((group_size,)),
                pltpu.SemaphoreType.DMA((group_size,)),
            ],
            compiler_params=pltpu.CompilerParams(collective_id=0, has_side_effects=True, vmem_limit_bytes=44 * 1024 * 1024),
        )(grid, unitaries.transpose(0, 2, 3, 1), cz_pairs.T)
        state, z_expect = pl.pallas_call(
            functools.partial(flush_kernel, 1.0 / 2 ** num_qubits),
            out_shape=(jax.ShapeDtypeStruct(shape, jnp.float32), jax.ShapeDtypeStruct((1, num_qubits), jnp.float32)),
            in_specs=[pl.BlockSpec(memory_space=pltpu.VMEM)] * 2,
            out_specs=(pl.BlockSpec(memory_space=pl.ANY), pl.BlockSpec(memory_space=pl.ANY)),
            scratch_shapes=[pltpu.VMEM((1, num_qubits), jnp.float32), pltpu.SemaphoreType.DMA((QUARTERS, FLUSH_PIECES)), pltpu.SemaphoreType.DMA],
            compiler_params=pltpu.CompilerParams(vmem_limit_bytes=2 ** 20),
        )(pltpu.with_memory_space_constraint(state, pltpu.VMEM), pltpu.with_memory_space_constraint(parts, pltpu.VMEM))
        state = state.reshape(row_count, 2, LANES).transpose(1, 0, 2).reshape(2, local_size)
        return state, z_expect.reshape(num_qubits)

    return jax.shard_map(local_layer, mesh=mesh, in_specs=(P(None, 'q'), P(), P()), out_specs=(P(None, 'q'), P()), check_vma=False)
```

```python
import functools
import jax
import jax.numpy as jnp
from jax import lax
from jax.experimental import pallas as pl
from jax.experimental.pallas import tpu as pltpu
from jax.sharding import PartitionSpec as P

MESH = pl.DeviceIdType.MESH
LANES = 128
LANE_BITS = 7
ROW_BITS = 7
MID_BITS = 5
QUARTERS = 4
BLOCKS = 2 ** MID_BITS
BLOCK_ROWS = 2 * 2 ** ROW_BITS
HALF = BLOCK_ROWS // 2
LOCAL_BLOCKS = 2
LOAD_SPANS = (1, 6, 9, 16)
LINK_SPANS = ((1, 6, 9, 16), (16, 16), (16, 16), (16, 9, 3))
SWAP_BLOCKS = (28, 29, 30, 31)
CORE_SPANS = (8, 8, 8, 8)
MAX_PIECES = 4
FLUSH_PIECES = 1
TOP_BITS = 4
CORE = 3
HI_BITS = 2 + MID_BITS
HIGHEST = lax.Precision.HIGHEST


def apply_coefs(coef_a, coef_b, first, second):
    out_re = coef_a[0] * first[0] - coef_a[1] * first[1] + coef_b[0] * second[0] - coef_b[1] * second[1]
    out_im = coef_a[0] * first[1] + coef_a[1] * first[0] + coef_b[0] * second[1] + coef_b[1] * second[0]
    return out_re, out_im


def gate_coefs(gates_ref, qubit):
    return [[(gates_ref[0, row, col, qubit], gates_ref[1, row, col, qubit]) for col in range(2)] for row in range(2)]


def pieces_of(spans):
    starts = [sum(spans[:pos]) for pos in range(len(spans))]
    return list(zip(starts, spans))


def butterfly(values, gates):
    size = len(values)
    for gate_pos, gate in enumerate(gates):
        stride = size >> (gate_pos + 1)
        values = list(values)
        for pos in range(size):
            if pos & stride:
                continue
            zero_half, one_half = values[pos], values[pos + stride]
            values[pos] = apply_coefs(gate[0][0], gate[0][1], zero_half, one_half)
            values[pos + stride] = apply_coefs(gate[1][0], gate[1][1], zero_half, one_half)
    return values


def load_rows(ref, row, rows):
    return ref[pl.ds(2 * row, rows, stride=2), :], ref[pl.ds(2 * row + 1, rows, stride=2), :]


def store_rows(ref, row, rows, value):
    ref[pl.ds(2 * row, rows, stride=2), :] = value[0]
    ref[pl.ds(2 * row + 1, rows, stride=2), :] = value[1]


def gate_blocks(refs, gates, rows):
    @pl.loop(0, HALF // rows)
    def _(group):
        row = pl.multiple_of(group * rows, rows)
        values = butterfly([load_rows(ref, row, rows) for ref in refs], gates)
        for ref, value in zip(refs, values):
            store_rows(ref, row, rows, value)


def build_matrix(mat_ref, gates_ref, first_qubit, num_bits, transposed):
    size = 2 ** num_bits
    out_index = lax.broadcasted_iota(jnp.int32, (size, size), 1 if transposed else 0)
    in_index = lax.broadcasted_iota(jnp.int32, (size, size), 0 if transposed else 1)
    prod_re = jnp.ones((size, size), jnp.float32)
    prod_im = jnp.zeros((size, size), jnp.float32)
    for bit_pos in range(num_bits):
        gate = gate_coefs(gates_ref, first_qubit + bit_pos)
        mask = 2 ** (num_bits - 1 - bit_pos)
        out_one = (out_index & mask) != 0
        in_one = (in_index & mask) != 0
        fac_re, fac_im = [jnp.where(out_one, jnp.where(in_one, gate[1][1][part], gate[1][0][part]), jnp.where(in_one, gate[0][1][part], gate[0][0][part])) for part in range(2)]
        prod_re, prod_im = prod_re * fac_re - prod_im * fac_im, prod_re * fac_im + prod_im * fac_re
    mat_ref[0:size, 0:size] = prod_re
    mat_ref[size:, size:] = prod_re
    mat_ref[0:size, size:] = prod_im if transposed else -prod_im
    mat_ref[size:, 0:size] = -prod_im if transposed else prod_im


def kernel(group_size, x_ref, gates_hbm, pairs_hbm, out_ref, parts_ref, recv_ref, lane_mat, row_mat, back_ref, low_sum, high_sum, sent_sum, part_ref,
           gates_ref, pairs_ref, mask_ref, small_sem, ready_sem, swap_sem, load_sem, send_sem, recv_sem, part_send, part_recv):
    num_qubits = gates_hbm.shape[3]
    num_pairs = pairs_hbm.shape[1]
    me = lax.axis_index('q')
    strides = [group_size >> (link + 1) for link in range(TOP_BITS)]
    own_bits = [(me // stride) % 2 for stride in strides]
    partners = [me + stride * (1 - 2 * own_bit) for stride, own_bit in zip(strides, own_bits)]

    load_pieces = pieces_of(LOAD_SPANS)
    link_pieces = [pieces_of(spans) for spans in LINK_SPANS]
    core_pieces = pieces_of(CORE_SPANS)

    def load(piece):
        span = pl.ds(*load_pieces[piece])
        return pltpu.make_async_copy(x_ref.at[:, span], out_ref.at[:, span], load_sem.at[piece])

    def exchange(link, slot, piece):
        span = pl.ds(*(core_pieces if link == CORE else link_pieces[slot])[piece])
        return pltpu.make_async_remote_copy(
            src_ref=out_ref.at[(slot + link) % 4, span], dst_ref=recv_ref.at[link, slot % 2, span],
            send_sem=send_sem.at[link, slot % 2, piece], recv_sem=recv_sem.at[link, slot % 2, piece],
            device_id=(partners[link],), device_id_type=MESH)

    def half_rows(bit):
        return pl.ds(pl.multiple_of(bit * HALF, HALF), HALF)

    def swap_out(link, swap):
        quarter, block, rows = (QUARTERS - 1 + link) % 4, SWAP_BLOCKS[swap], half_rows(1 - own_bits[link])
        return pltpu.make_async_remote_copy(
            src_ref=out_ref.at[quarter, block, rows], dst_ref=recv_ref.at[link, 1, block, rows],
            send_sem=swap_sem.at[0, link, swap], recv_sem=swap_sem.at[1, link, swap], device_id=(partners[link],), device_id_type=MESH)

    def swap_back(link, swap):
        return pltpu.make_async_remote_copy(
            src_ref=recv_ref.at[link, 1, SWAP_BLOCKS[swap], half_rows(own_bits[link])], dst_ref=back_ref.at[link, swap],
            send_sem=swap_sem.at[2, link, swap], recv_sem=swap_sem.at[3, link, swap], device_id=(partners[link],), device_id_type=MESH)

    def send_links(slot, done_from, done_to):
        for piece, (start, size) in enumerate(link_pieces[slot]):
            if done_from < start + size <= done_to:
                for link in range(CORE):
                    exchange(link, slot, piece).start()
        if slot == QUARTERS - 1:
            for swap, block in enumerate(SWAP_BLOCKS):
                if done_from <= block < done_to:
                    for link in range(CORE):
                        swap_out(link, swap).start()

    barrier = pltpu.get_barrier_semaphore()
    for partner in partners:
        pl.semaphore_signal(barrier, inc=1, device_id=(partner,), device_id_type=MESH)
    small = [pltpu.make_async_copy(gates_hbm, gates_ref, small_sem.at[0]), pltpu.make_async_copy(pairs_hbm, pairs_ref, small_sem.at[1])]
    load(0).start()
    for copy in small:
        copy.start()
    for piece in range(1, len(load_pieces)):
        load(piece).start()
    for copy in small:
        copy.wait()

    quarter_gates = [gate_coefs(gates_ref, TOP_BITS), gate_coefs(gates_ref, TOP_BITS + 1)]

    for piece, (start, size) in enumerate(load_pieces):
        load(piece).wait()

        @pl.loop(start, start + size)
        def _(block):
            gate_blocks([out_ref.at[quarter, block] for quarter in range(QUARTERS)], quarter_gates, 16)

        if piece == 0:
            pl.semaphore_wait(barrier, TOP_BITS)
        send_links(0, start, start + size)

    def mid_gates(quarter):
        first = TOP_BITS + 2
        gates = [gate_coefs(gates_ref, first + bit_pos) for bit_pos in range(MID_BITS)]

        @pl.loop(0, BLOCKS // 8)
        def _(low):
            gate_blocks([out_ref.at[quarter, pos * (BLOCKS // 8) + low] for pos in range(8)], gates[:3], 8)

        @pl.loop(0, BLOCKS // 4)
        def _(high):
            gate_blocks([out_ref.at[quarter, high * 4 + pos] for pos in range(4)], gates[3:], 16)

    def finish(target_ref, device, quarter, block, row, rows, value):
        first_row = ((device * QUARTERS + quarter) * BLOCKS + block) * HALF + row
        index = first_row * LANES + lax.broadcasted_iota(jnp.int32, (rows, LANES), 0) * LANES + lax.broadcasted_iota(jnp.int32, (rows, LANES), 1)
        odd = None
        for pair_pos in range(num_pairs):
            mask = mask_ref[pair_pos]
            hit = (index & mask) == mask
            odd = hit if odd is None else jnp.logical_xor(odd, hit)
        sign = jnp.where(odd, -1.0, 1.0)
        value = (value[0] * sign, value[1] * sign)
        store_rows(target_ref, row, rows, value)
        density = value[0] * value[0] + value[1] * value[1]
        low_sum[pl.ds(row, rows), :] += density
        return jnp.sum(density.reshape(rows // 8, 8, LANES), axis=0)

    def add_high(quarter, block, total):
        position = quarter * BLOCKS + block
        for bit_pos in range(HI_BITS):
            bit = (position // 2 ** (HI_BITS - 1 - bit_pos)) % 2
            high_sum[bit_pos] += total * jnp.asarray(1 - 2 * bit, jnp.float32)
        high_sum[HI_BITS] += total

    def mix(link, slot, block, last):
        quarter = (slot + link) % 4
        own_bit = own_bits[link]
        coef_self = [gates_ref[part, own_bit, own_bit, link] for part in range(2)]
        coef_other = [gates_ref[part, own_bit, 1 - own_bit, link] for part in range(2)]
        rows = 32
        own_ref = out_ref.at[quarter, block]
        other_ref = recv_ref.at[link, slot % 2, block]

        def body(group, total):
            row = pl.multiple_of(group * rows, rows)
            value = apply_coefs(coef_self, coef_other, load_rows(own_ref, row, rows), load_rows(other_ref, row, rows))
            if last:
                return total + finish(own_ref, me, quarter, block, row, rows, value)
            store_rows(own_ref, row, rows, value)
            return total

        total = lax.fori_loop(0, HALF // rows, body, jnp.zeros((8, LANES), jnp.float32))
        if last:
            add_high(quarter, block, total)

    def mix_swap(link, swap):
        quarter, block = (QUARTERS - 1 + link) % 4, SWAP_BLOCKS[swap]
        own_bit = own_bits[link]
        home, away = [[[gates_ref[part, row_bit, col_bit, link] for part in range(2)] for col_bit in (own_bit, 1 - own_bit)] for row_bit in (own_bit, 1 - own_bit)]
        rows = 32
        own_ref = out_ref.at[quarter, block]
        other_ref = recv_ref.at[link, 1, block]

        def body(group, totals):
            row = pl.multiple_of(own_bit * (HALF // 2) + group * rows, rows)
            own, other = load_rows(own_ref, row, rows), load_rows(other_ref, row, rows)
            kept = finish(own_ref, me, quarter, block, row, rows, apply_coefs(home[0], home[1], own, other))
            sent = finish(other_ref, partners[link], quarter, block, row, rows, apply_coefs(away[0], away[1], own, other))
            return totals[0] + kept, totals[1] + sent

        zero = jnp.zeros((8, LANES), jnp.float32)
        kept, sent = lax.fori_loop(0, HALF // 2 // rows, body, (zero, zero))
        add_high(quarter, block, kept + sent)
        sent_sum[link] += sent

    def local(slot, first_block, last):
        quarter = (slot + CORE) % 4
        blocks = [first_block + pos for pos in range(LOCAL_BLOCKS)]
        for block in blocks:
            mix(CORE, slot, block, False)
        refs = [out_ref.at[quarter, block] for block in blocks]
        parts = [load_rows(ref, 0, HALF) for ref in refs]
        rows = jnp.concatenate([jnp.concatenate(part, axis=1) for part in parts], axis=0)
        mixed = jnp.dot(rows, lane_mat[...], precision=HIGHEST, preferred_element_type=jnp.float32)
        columns = jnp.concatenate([
            jnp.concatenate([mixed[pos * HALF:(pos + 1) * HALF, :LANES], mixed[pos * HALF:(pos + 1) * HALF, LANES:]], axis=0)
            for pos in range(LOCAL_BLOCKS)], axis=1)
        done = jnp.dot(row_mat[...], columns, precision=HIGHEST, preferred_element_type=jnp.float32)
        for pos, ref in enumerate(refs):
            piece = done[:, pos * LANES:(pos + 1) * LANES]
            store_rows(ref, 0, HALF, (piece[:HALF], piece[HALF:]))
        if last:
            group_rows = 32
            for block in blocks:
                def body(group, total):
                    row = pl.multiple_of(group * group_rows, group_rows)
                    return total + finish(out_ref.at[quarter, block], me, quarter, block, row, group_rows, load_rows(out_ref.at[quarter, block], row, group_rows))

                total = lax.fori_loop(0, HALF // group_rows, body, jnp.zeros((8, LANES), jnp.float32))
                add_high(quarter, block, total)

    for pair_pos in range(num_pairs):
        mask_ref[pair_pos] = (1 << (num_qubits - 1 - pairs_ref[0, pair_pos])) | (1 << (num_qubits - 1 - pairs_ref[1, pair_pos]))
    low_sum[...] = jnp.zeros_like(low_sum)
    high_sum[...] = jnp.zeros_like(high_sum)
    sent_sum[...] = jnp.zeros_like(sent_sum)
    for link, partner in enumerate(partners):
        pl.semaphore_signal(ready_sem.at[link], inc=1, device_id=(partner,), device_id_type=MESH)
        pl.semaphore_wait(ready_sem.at[link], 1)
    build_matrix(lane_mat, gates_ref, num_qubits - LANE_BITS, LANE_BITS, True)
    build_matrix(row_mat, gates_ref, num_qubits - LANE_BITS - ROW_BITS, ROW_BITS, False)
    for slot in range(QUARTERS):
        last = slot == QUARTERS - 1
        mid_gates((slot + CORE) % 4)
        for piece in range(len(core_pieces)):
            exchange(CORE, slot, piece).start()
        for piece, (start, size) in enumerate(core_pieces):
            copy = exchange(CORE, slot, piece)
            copy.wait_recv()
            copy.wait_send()

            @pl.loop(start // LOCAL_BLOCKS, (start + size) // LOCAL_BLOCKS)
            def _(step):
                local(slot, step * LOCAL_BLOCKS, last)

        for piece, (start, size) in enumerate(link_pieces[slot]):
            for link in range(CORE):
                copy = exchange(link, slot, piece)
                copy.wait_recv()
                copy.wait_send()

                @pl.loop(start, start + size)
                def _(block):
                    mix(link, slot, block, last)

            if not last:
                send_links(slot + 1, start, start + size)

    for swap in range(len(SWAP_BLOCKS)):
        for link in range(CORE):
            copy = swap_out(link, swap)
            copy.wait_recv()
            copy.wait_send()
            mix_swap(link, swap)
        if swap < len(SWAP_BLOCKS) - 1:
            for link in range(CORE):
                swap_back(link, swap).start()

    total = high_sum[HI_BITS]
    sublane = lax.broadcasted_iota(jnp.int32, (8, LANES), 0)
    lane = lax.broadcasted_iota(jnp.int32, (8, LANES), 1)
    signed = [(total - 2.0 * sent_sum[link]) * (1 - 2 * own_bit).astype(jnp.float32) for link, own_bit in enumerate(own_bits)]
    signed += [high_sum[bit_pos] for bit_pos in range(HI_BITS)]
    low = [low_sum[8 * pos:8 * pos + 8, :] for pos in range(HALF // 8)]
    for bit_pos in range(ROW_BITS - 3):
        mask = 2 ** (ROW_BITS - 4 - bit_pos)
        signed.append(functools.reduce(jnp.add, [-part if pos & mask else part for pos, part in enumerate(low)]))
    signed += [jnp.where((sublane & (4 >> bit_pos)) != 0, -total, total) for bit_pos in range(3)]
    signed += [jnp.where((lane & (64 >> bit_pos)) != 0, -total, total) for bit_pos in range(LANE_BITS)]
    rows = [jnp.sum(part, axis=0, keepdims=True) for part in signed]
    table = jnp.concatenate(rows + [jnp.zeros((LANES - len(rows), LANES), jnp.float32)], axis=0)
    part = lax.dot_general(jnp.ones((8, LANES), jnp.float32), table, (((1,), (1,)), ((), ())), precision=HIGHEST, preferred_element_type=jnp.float32)
    part_ref[0] = part

    chips = group_size // 2
    pair = pltpu.make_async_remote_copy(
        src_ref=part_ref.at[0], dst_ref=part_ref.at[1], send_sem=part_send.at[0], recv_sem=part_recv.at[chips],
        device_id=(partners[CORE],), device_id_type=MESH)
    pair.start()
    pair.wait_recv()
    chip_part = part + part_ref[1]
    part_ref[2] = chip_part

    def share(offset, slot):
        return pltpu.make_async_remote_copy(
            src_ref=part_ref.at[2, pl.ds(0, 1)], dst_ref=parts_ref.at[slot, pl.ds(0, 1)], send_sem=part_send.at[offset], recv_sem=part_recv.at[slot],
            device_id=((me + 2 * offset) % group_size,), device_id_type=MESH)

    for offset in range(1, chips):
        share(offset, me // 2).start()
    parts_ref[me // 2] = chip_part

    def send_last():
        for link in range(CORE):
            swap_back(link, len(SWAP_BLOCKS) - 1).start()

    def take_back(swap):
        for link in range(CORE):
            copy = swap_back(link, swap)
            copy.wait_recv()
            out_ref[(QUARTERS - 1 + link) % 4, SWAP_BLOCKS[swap], half_rows(1 - own_bits[link]), :] = back_ref[link, swap]
            copy.wait_send()

    pl.when(own_bits[CORE] == 0)(send_last)
    for swap in range(len(SWAP_BLOCKS) - 1):
        take_back(swap)
    pl.when(own_bits[CORE] != 0)(send_last)
    take_back(len(SWAP_BLOCKS) - 1)
    pair.wait_send()
    for offset in range(1, chips):
        share(offset, (me // 2 + chips - offset) % chips).wait_recv()
    for offset in range(1, chips):
        share(offset, me // 2).wait_send()


def flush_kernel(scale, state_ref, parts_ref, out_ref, z_hbm, z_ref, sem, z_sem):
    size = BLOCKS // FLUSH_PIECES
    copies = []
    for quarter in range(QUARTERS):
        for piece in range(FLUSH_PIECES):
            span = pl.ds(piece * size, size)
            copies.append(pltpu.make_async_copy(state_ref.at[quarter, span], out_ref.at[quarter, span], sem.at[quarter, piece]))
    for copy in copies:
        copy.start()
    total = functools.reduce(jnp.add, [parts_ref[pos, 0:1, :] for pos in range(parts_ref.shape[0])])
    z_ref[...] = total[:, :z_ref.shape[1]] * scale
    copies.append(pltpu.make_async_copy(z_ref, z_hbm, z_sem))
    copies[-1].start()
    for copy in copies:
        copy.wait()


def solution(mesh):
    group_size = mesh.shape['q']

    def local_layer(state_local, unitaries, cz_pairs):
        num_qubits = unitaries.shape[1]
        local_size = state_local.shape[1]
        row_count = local_size // LANES
        shape = (QUARTERS, BLOCKS, BLOCK_ROWS, LANES)
        grid = state_local.reshape(2, row_count, LANES).transpose(1, 0, 2).reshape(shape)
        state, parts = pl.pallas_call(
            functools.partial(kernel, group_size),
            out_shape=(pltpu.VMEM(shape, jnp.float32), pltpu.VMEM((group_size // 2, 8, LANES), jnp.float32)),
            in_specs=[pl.BlockSpec(memory_space=pl.ANY)] * 3,
            out_specs=(pl.BlockSpec(memory_space=pltpu.VMEM), pl.BlockSpec(memory_space=pltpu.VMEM)),
            scratch_shapes=[
                pltpu.VMEM((TOP_BITS, 2, BLOCKS, BLOCK_ROWS, LANES), jnp.float32),
                pltpu.VMEM((2 * LANES, 2 * LANES), jnp.float32),
                pltpu.VMEM((BLOCK_ROWS, BLOCK_ROWS), jnp.float32),
                pltpu.VMEM((CORE, len(SWAP_BLOCKS), HALF, LANES), jnp.float32),
                pltpu.VMEM((HALF, LANES), jnp.float32),
                pltpu.VMEM((HI_BITS + 1, 8, LANES), jnp.float32),
                pltpu.VMEM((TOP_BITS, 8, LANES), jnp.float32),
                pltpu.VMEM((3, 8, LANES), jnp.float32),
                pltpu.SMEM((2, 2, 2, num_qubits), jnp.float32),
                pltpu.SMEM((2, cz_pairs.shape[0]), jnp.int32),
                pltpu.SMEM((cz_pairs.shape[0],), jnp.int32),
                pltpu.SemaphoreType.DMA((2,)),
                pltpu.SemaphoreType.REGULAR((TOP_BITS,)),
                pltpu.SemaphoreType.DMA((4, CORE, len(SWAP_BLOCKS))),
                pltpu.SemaphoreType.DMA((len(LOAD_SPANS),)),
                pltpu.SemaphoreType.DMA((TOP_BITS, 2, MAX_PIECES)),
                pltpu.SemaphoreType.DMA((TOP_BITS, 2, MAX_PIECES)),
                pltpu.SemaphoreType.DMA((group_size,)),
                pltpu.SemaphoreType.DMA((group_size,)),
            ],
            compiler_params=pltpu.CompilerParams(collective_id=0, has_side_effects=True, vmem_limit_bytes=44 * 1024 * 1024),
        )(grid, unitaries.transpose(0, 2, 3, 1), cz_pairs.T)
        state, z_expect = pl.pallas_call(
            functools.partial(flush_kernel, 1.0 / 2 ** num_qubits),
            out_shape=(jax.ShapeDtypeStruct(shape, jnp.float32), jax.ShapeDtypeStruct((1, num_qubits), jnp.float32)),
            in_specs=[pl.BlockSpec(memory_space=pltpu.VMEM)] * 2,
            out_specs=(pl.BlockSpec(memory_space=pl.ANY), pl.BlockSpec(memory_space=pl.ANY)),
            scratch_shapes=[pltpu.VMEM((1, num_qubits), jnp.float32), pltpu.SemaphoreType.DMA((QUARTERS, FLUSH_PIECES)), pltpu.SemaphoreType.DMA],
            compiler_params=pltpu.CompilerParams(vmem_limit_bytes=2 ** 20),
        )(pltpu.with_memory_space_constraint(state, pltpu.VMEM), pltpu.with_memory_space_constraint(parts, pltpu.VMEM))
        state = state.reshape(row_count, 2, LANES).transpose(1, 0, 2).reshape(2, local_size)
        return state, z_expect.reshape(num_qubits)

    return jax.shard_map(local_layer, mesh=mesh, in_specs=(P(None, 'q'), P(), P()), out_specs=(P(None, 'q'), P()), check_vma=False)
```

```python
import functools
import jax
import jax.numpy as jnp
from jax import lax
from jax.experimental import pallas as pl
from jax.experimental.pallas import tpu as pltpu
from jax.sharding import PartitionSpec as P

MESH = pl.DeviceIdType.MESH
LANES = 128
LANE_BITS = 7
ROW_BITS = 7
MID_BITS = 5
QUARTERS = 4
BLOCKS = 2 ** MID_BITS
BLOCK_ROWS = 2 * 2 ** ROW_BITS
HALF = BLOCK_ROWS // 2
LOCAL_BLOCKS = 2
LOAD_SPANS = (1, 7, 24)
LINK_SPANS = ((1, 7, 24), (8, 24), (8, 24), (8, 17, 3))
SWAP_BLOCKS = (28, 29, 30, 31)
CORE_SPANS = (8, 8, 8, 8)
MAX_PIECES = 4
FLUSH_PIECES = 1
TOP_BITS = 4
CORE = 3
HI_BITS = 2 + MID_BITS
HIGHEST = lax.Precision.HIGHEST


def apply_coefs(coef_a, coef_b, first, second):
    out_re = coef_a[0] * first[0] - coef_a[1] * first[1] + coef_b[0] * second[0] - coef_b[1] * second[1]
    out_im = coef_a[0] * first[1] + coef_a[1] * first[0] + coef_b[0] * second[1] + coef_b[1] * second[0]
    return out_re, out_im


def gate_coefs(gates_ref, qubit):
    return [[(gates_ref[0, row, col, qubit], gates_ref[1, row, col, qubit]) for col in range(2)] for row in range(2)]


def pieces_of(spans):
    starts = [sum(spans[:pos]) for pos in range(len(spans))]
    return list(zip(starts, spans))


def butterfly(values, gates):
    size = len(values)
    for gate_pos, gate in enumerate(gates):
        stride = size >> (gate_pos + 1)
        values = list(values)
        for pos in range(size):
            if pos & stride:
                continue
            zero_half, one_half = values[pos], values[pos + stride]
            values[pos] = apply_coefs(gate[0][0], gate[0][1], zero_half, one_half)
            values[pos + stride] = apply_coefs(gate[1][0], gate[1][1], zero_half, one_half)
    return values


def load_rows(ref, row, rows):
    return ref[pl.ds(2 * row, rows, stride=2), :], ref[pl.ds(2 * row + 1, rows, stride=2), :]


def store_rows(ref, row, rows, value):
    ref[pl.ds(2 * row, rows, stride=2), :] = value[0]
    ref[pl.ds(2 * row + 1, rows, stride=2), :] = value[1]


def gate_blocks(refs, gates, rows):
    @pl.loop(0, HALF // rows)
    def _(group):
        row = pl.multiple_of(group * rows, rows)
        values = butterfly([load_rows(ref, row, rows) for ref in refs], gates)
        for ref, value in zip(refs, values):
            store_rows(ref, row, rows, value)


def build_matrix(mat_ref, gates_ref, first_qubit, num_bits, transposed):
    size = 2 ** num_bits
    out_index = lax.broadcasted_iota(jnp.int32, (size, size), 1 if transposed else 0)
    in_index = lax.broadcasted_iota(jnp.int32, (size, size), 0 if transposed else 1)
    prod_re = jnp.ones((size, size), jnp.float32)
    prod_im = jnp.zeros((size, size), jnp.float32)
    for bit_pos in range(num_bits):
        gate = gate_coefs(gates_ref, first_qubit + bit_pos)
        mask = 2 ** (num_bits - 1 - bit_pos)
        out_one = (out_index & mask) != 0
        in_one = (in_index & mask) != 0
        fac_re, fac_im = [jnp.where(out_one, jnp.where(in_one, gate[1][1][part], gate[1][0][part]), jnp.where(in_one, gate[0][1][part], gate[0][0][part])) for part in range(2)]
        prod_re, prod_im = prod_re * fac_re - prod_im * fac_im, prod_re * fac_im + prod_im * fac_re
    mat_ref[0:size, 0:size] = prod_re
    mat_ref[size:, size:] = prod_re
    mat_ref[0:size, size:] = prod_im if transposed else -prod_im
    mat_ref[size:, 0:size] = -prod_im if transposed else prod_im


def kernel(group_size, x_ref, gates_hbm, pairs_hbm, out_ref, parts_ref, recv_ref, lane_mat, row_mat, back_ref, low_sum, high_sum, sent_sum, part_ref,
           gates_ref, pairs_ref, mask_ref, small_sem, ready_sem, swap_sem, load_sem, send_sem, recv_sem, part_send, part_recv):
    num_qubits = gates_hbm.shape[3]
    num_pairs = pairs_hbm.shape[1]
    me = lax.axis_index('q')
    strides = [group_size >> (link + 1) for link in range(TOP_BITS)]
    own_bits = [(me // stride) % 2 for stride in strides]
    partners = [me + stride * (1 - 2 * own_bit) for stride, own_bit in zip(strides, own_bits)]

    load_pieces = pieces_of(LOAD_SPANS)
    link_pieces = [pieces_of(spans) for spans in LINK_SPANS]
    core_pieces = pieces_of(CORE_SPANS)

    def load(piece):
        span = pl.ds(*load_pieces[piece])
        return pltpu.make_async_copy(x_ref.at[:, span], out_ref.at[:, span], load_sem.at[piece])

    def exchange(link, slot, piece):
        span = pl.ds(*(core_pieces if link == CORE else link_pieces[slot])[piece])
        return pltpu.make_async_remote_copy(
            src_ref=out_ref.at[(slot + link) % 4, span], dst_ref=recv_ref.at[link, slot % 2, span],
            send_sem=send_sem.at[link, slot % 2, piece], recv_sem=recv_sem.at[link, slot % 2, piece],
            device_id=(partners[link],), device_id_type=MESH)

    def half_rows(bit):
        return pl.ds(pl.multiple_of(bit * HALF, HALF), HALF)

    def swap_out(link, swap):
        quarter, block, rows = (QUARTERS - 1 + link) % 4, SWAP_BLOCKS[swap], half_rows(1 - own_bits[link])
        return pltpu.make_async_remote_copy(
            src_ref=out_ref.at[quarter, block, rows], dst_ref=recv_ref.at[link, 1, block, rows],
            send_sem=swap_sem.at[0, link, swap], recv_sem=swap_sem.at[1, link, swap], device_id=(partners[link],), device_id_type=MESH)

    def swap_back(link, swap):
        return pltpu.make_async_remote_copy(
            src_ref=recv_ref.at[link, 1, SWAP_BLOCKS[swap], half_rows(own_bits[link])], dst_ref=back_ref.at[link, swap],
            send_sem=swap_sem.at[2, link, swap], recv_sem=swap_sem.at[3, link, swap], device_id=(partners[link],), device_id_type=MESH)

    def send_links(slot, done_from, done_to):
        for piece, (start, size) in enumerate(link_pieces[slot]):
            if done_from < start + size <= done_to:
                for link in range(CORE):
                    exchange(link, slot, piece).start()
        if slot == QUARTERS - 1:
            for swap, block in enumerate(SWAP_BLOCKS):
                if done_from <= block < done_to:
                    for link in range(CORE):
                        swap_out(link, swap).start()

    barrier = pltpu.get_barrier_semaphore()
    for partner in partners:
        pl.semaphore_signal(barrier, inc=1, device_id=(partner,), device_id_type=MESH)
    small = [pltpu.make_async_copy(gates_hbm, gates_ref, small_sem.at[0]), pltpu.make_async_copy(pairs_hbm, pairs_ref, small_sem.at[1])]
    load(0).start()
    for copy in small:
        copy.start()
    for piece in range(1, len(load_pieces)):
        load(piece).start()
    for copy in small:
        copy.wait()

    quarter_gates = [gate_coefs(gates_ref, TOP_BITS), gate_coefs(gates_ref, TOP_BITS + 1)]

    for piece, (start, size) in enumerate(load_pieces):
        load(piece).wait()

        @pl.loop(start, start + size)
        def _(block):
            gate_blocks([out_ref.at[quarter, block] for quarter in range(QUARTERS)], quarter_gates, 16)

        if piece == 0:
            pl.semaphore_wait(barrier, TOP_BITS)
        send_links(0, start, start + size)

    def mid_gates(quarter):
        first = TOP_BITS + 2
        gates = [gate_coefs(gates_ref, first + bit_pos) for bit_pos in range(MID_BITS)]

        @pl.loop(0, BLOCKS // 8)
        def _(low):
            gate_blocks([out_ref.at[quarter, pos * (BLOCKS // 8) + low] for pos in range(8)], gates[:3], 8)

        @pl.loop(0, BLOCKS // 4)
        def _(high):
            gate_blocks([out_ref.at[quarter, high * 4 + pos] for pos in range(4)], gates[3:], 16)

    def finish(target_ref, device, quarter, block, row, rows, value):
        first_row = ((device * QUARTERS + quarter) * BLOCKS + block) * HALF + row
        index = first_row * LANES + lax.broadcasted_iota(jnp.int32, (rows, LANES), 0) * LANES + lax.broadcasted_iota(jnp.int32, (rows, LANES), 1)
        odd = None
        for pair_pos in range(num_pairs):
            mask = mask_ref[pair_pos]
            hit = (index & mask) == mask
            odd = hit if odd is None else jnp.logical_xor(odd, hit)
        sign = jnp.where(odd, -1.0, 1.0)
        value = (value[0] * sign, value[1] * sign)
        store_rows(target_ref, row, rows, value)
        density = value[0] * value[0] + value[1] * value[1]
        low_sum[pl.ds(row, rows), :] += density
        return jnp.sum(density.reshape(rows // 8, 8, LANES), axis=0)

    def add_high(quarter, block, total):
        position = quarter * BLOCKS + block
        for bit_pos in range(HI_BITS):
            bit = (position // 2 ** (HI_BITS - 1 - bit_pos)) % 2
            high_sum[bit_pos] += total * jnp.asarray(1 - 2 * bit, jnp.float32)
        high_sum[HI_BITS] += total

    def mix(link, slot, block, last):
        quarter = (slot + link) % 4
        own_bit = own_bits[link]
        coef_self = [gates_ref[part, own_bit, own_bit, link] for part in range(2)]
        coef_other = [gates_ref[part, own_bit, 1 - own_bit, link] for part in range(2)]
        rows = 32
        own_ref = out_ref.at[quarter, block]
        other_ref = recv_ref.at[link, slot % 2, block]

        def body(group, total):
            row = pl.multiple_of(group * rows, rows)
            value = apply_coefs(coef_self, coef_other, load_rows(own_ref, row, rows), load_rows(other_ref, row, rows))
            if last:
                return total + finish(own_ref, me, quarter, block, row, rows, value)
            store_rows(own_ref, row, rows, value)
            return total

        total = lax.fori_loop(0, HALF // rows, body, jnp.zeros((8, LANES), jnp.float32))
        if last:
            add_high(quarter, block, total)

    def mix_swap(link, swap):
        quarter, block = (QUARTERS - 1 + link) % 4, SWAP_BLOCKS[swap]
        own_bit = own_bits[link]
        home, away = [[[gates_ref[part, row_bit, col_bit, link] for part in range(2)] for col_bit in (own_bit, 1 - own_bit)] for row_bit in (own_bit, 1 - own_bit)]
        rows = 32
        own_ref = out_ref.at[quarter, block]
        other_ref = recv_ref.at[link, 1, block]

        def body(group, totals):
            row = pl.multiple_of(own_bit * (HALF // 2) + group * rows, rows)
            own, other = load_rows(own_ref, row, rows), load_rows(other_ref, row, rows)
            kept = finish(own_ref, me, quarter, block, row, rows, apply_coefs(home[0], home[1], own, other))
            sent = finish(other_ref, partners[link], quarter, block, row, rows, apply_coefs(away[0], away[1], own, other))
            return totals[0] + kept, totals[1] + sent

        zero = jnp.zeros((8, LANES), jnp.float32)
        kept, sent = lax.fori_loop(0, HALF // 2 // rows, body, (zero, zero))
        add_high(quarter, block, kept + sent)
        sent_sum[link] += sent

    def local(slot, first_block, last):
        quarter = (slot + CORE) % 4
        blocks = [first_block + pos for pos in range(LOCAL_BLOCKS)]
        for block in blocks:
            mix(CORE, slot, block, False)
        refs = [out_ref.at[quarter, block] for block in blocks]
        parts = [load_rows(ref, 0, HALF) for ref in refs]
        rows = jnp.concatenate([jnp.concatenate(part, axis=1) for part in parts], axis=0)
        mixed = jnp.dot(rows, lane_mat[...], precision=HIGHEST, preferred_element_type=jnp.float32)
        columns = jnp.concatenate([
            jnp.concatenate([mixed[pos * HALF:(pos + 1) * HALF, :LANES], mixed[pos * HALF:(pos + 1) * HALF, LANES:]], axis=0)
            for pos in range(LOCAL_BLOCKS)], axis=1)
        done = jnp.dot(row_mat[...], columns, precision=HIGHEST, preferred_element_type=jnp.float32)
        for pos, ref in enumerate(refs):
            piece = done[:, pos * LANES:(pos + 1) * LANES]
            store_rows(ref, 0, HALF, (piece[:HALF], piece[HALF:]))
        if last:
            group_rows = 32
            for block in blocks:
                def body(group, total):
                    row = pl.multiple_of(group * group_rows, group_rows)
                    return total + finish(out_ref.at[quarter, block], me, quarter, block, row, group_rows, load_rows(out_ref.at[quarter, block], row, group_rows))

                total = lax.fori_loop(0, HALF // group_rows, body, jnp.zeros((8, LANES), jnp.float32))
                add_high(quarter, block, total)

    for pair_pos in range(num_pairs):
        mask_ref[pair_pos] = (1 << (num_qubits - 1 - pairs_ref[0, pair_pos])) | (1 << (num_qubits - 1 - pairs_ref[1, pair_pos]))
    low_sum[...] = jnp.zeros_like(low_sum)
    high_sum[...] = jnp.zeros_like(high_sum)
    sent_sum[...] = jnp.zeros_like(sent_sum)
    for link, partner in enumerate(partners):
        pl.semaphore_signal(ready_sem.at[link], inc=1, device_id=(partner,), device_id_type=MESH)
        pl.semaphore_wait(ready_sem.at[link], 1)
    build_matrix(lane_mat, gates_ref, num_qubits - LANE_BITS, LANE_BITS, True)
    build_matrix(row_mat, gates_ref, num_qubits - LANE_BITS - ROW_BITS, ROW_BITS, False)
    for slot in range(QUARTERS):
        last = slot == QUARTERS - 1
        mid_gates((slot + CORE) % 4)
        for piece in range(len(core_pieces)):
            exchange(CORE, slot, piece).start()
        for piece, (start, size) in enumerate(core_pieces):
            copy = exchange(CORE, slot, piece)
            copy.wait_recv()
            copy.wait_send()

            @pl.loop(start // LOCAL_BLOCKS, (start + size) // LOCAL_BLOCKS)
            def _(step):
                local(slot, step * LOCAL_BLOCKS, last)

        for piece, (start, size) in enumerate(link_pieces[slot]):
            for link in range(CORE):
                copy = exchange(link, slot, piece)
                copy.wait_recv()
                copy.wait_send()

                @pl.loop(start, start + size)
                def _(block):
                    mix(link, slot, block, last)

            if not last:
                send_links(slot + 1, start, start + size)

    for swap in range(len(SWAP_BLOCKS)):
        for link in range(CORE):
            copy = swap_out(link, swap)
            copy.wait_recv()
            copy.wait_send()
            mix_swap(link, swap)
        if swap < len(SWAP_BLOCKS) - 1:
            for link in range(CORE):
                swap_back(link, swap).start()

    total = high_sum[HI_BITS]
    sublane = lax.broadcasted_iota(jnp.int32, (8, LANES), 0)
    lane = lax.broadcasted_iota(jnp.int32, (8, LANES), 1)
    signed = [(total - 2.0 * sent_sum[link]) * (1 - 2 * own_bit).astype(jnp.float32) for link, own_bit in enumerate(own_bits)]
    signed += [high_sum[bit_pos] for bit_pos in range(HI_BITS)]
    low = [low_sum[8 * pos:8 * pos + 8, :] for pos in range(HALF // 8)]
    for bit_pos in range(ROW_BITS - 3):
        mask = 2 ** (ROW_BITS - 4 - bit_pos)
        signed.append(functools.reduce(jnp.add, [-part if pos & mask else part for pos, part in enumerate(low)]))
    signed += [jnp.where((sublane & (4 >> bit_pos)) != 0, -total, total) for bit_pos in range(3)]
    signed += [jnp.where((lane & (64 >> bit_pos)) != 0, -total, total) for bit_pos in range(LANE_BITS)]
    rows = [jnp.sum(part, axis=0, keepdims=True) for part in signed]
    table = jnp.concatenate(rows + [jnp.zeros((LANES - len(rows), LANES), jnp.float32)], axis=0)
    part = lax.dot_general(jnp.ones((8, LANES), jnp.float32), table, (((1,), (1,)), ((), ())), precision=HIGHEST, preferred_element_type=jnp.float32)
    part_ref[0] = part

    chips = group_size // 2
    pair = pltpu.make_async_remote_copy(
        src_ref=part_ref.at[0], dst_ref=part_ref.at[1], send_sem=part_send.at[0], recv_sem=part_recv.at[chips],
        device_id=(partners[CORE],), device_id_type=MESH)
    pair.start()
    pair.wait_recv()
    chip_part = part + part_ref[1]
    part_ref[2] = chip_part

    def share(offset, slot):
        return pltpu.make_async_remote_copy(
            src_ref=part_ref.at[2, pl.ds(0, 1)], dst_ref=parts_ref.at[slot, pl.ds(0, 1)], send_sem=part_send.at[offset], recv_sem=part_recv.at[slot],
            device_id=((me + 2 * offset) % group_size,), device_id_type=MESH)

    for offset in range(1, chips):
        share(offset, me // 2).start()
    parts_ref[me // 2] = chip_part

    def send_last():
        for link in range(CORE):
            swap_back(link, len(SWAP_BLOCKS) - 1).start()

    def take_back(swap):
        for link in range(CORE):
            copy = swap_back(link, swap)
            copy.wait_recv()
            out_ref[(QUARTERS - 1 + link) % 4, SWAP_BLOCKS[swap], half_rows(1 - own_bits[link]), :] = back_ref[link, swap]
            copy.wait_send()

    pl.when(own_bits[CORE] == 0)(send_last)
    for swap in range(len(SWAP_BLOCKS) - 1):
        take_back(swap)
    pl.when(own_bits[CORE] != 0)(send_last)
    take_back(len(SWAP_BLOCKS) - 1)
    pair.wait_send()
    for offset in range(1, chips):
        share(offset, (me // 2 + chips - offset) % chips).wait_recv()
    for offset in range(1, chips):
        share(offset, me // 2).wait_send()


def flush_kernel(scale, state_ref, parts_ref, out_ref, z_hbm, z_ref, sem, z_sem):
    size = BLOCKS // FLUSH_PIECES
    copies = []
    for quarter in range(QUARTERS):
        for piece in range(FLUSH_PIECES):
            span = pl.ds(piece * size, size)
            copies.append(pltpu.make_async_copy(state_ref.at[quarter, span], out_ref.at[quarter, span], sem.at[quarter, piece]))
    for copy in copies:
        copy.start()
    total = functools.reduce(jnp.add, [parts_ref[pos, 0:1, :] for pos in range(parts_ref.shape[0])])
    z_ref[...] = total[:, :z_ref.shape[1]] * scale
    copies.append(pltpu.make_async_copy(z_ref, z_hbm, z_sem))
    copies[-1].start()
    for copy in copies:
        copy.wait()


def solution(mesh):
    group_size = mesh.shape['q']

    def local_layer(state_local, unitaries, cz_pairs):
        num_qubits = unitaries.shape[1]
        local_size = state_local.shape[1]
        row_count = local_size // LANES
        shape = (QUARTERS, BLOCKS, BLOCK_ROWS, LANES)
        grid = state_local.reshape(2, row_count, LANES).transpose(1, 0, 2).reshape(shape)
        state, parts = pl.pallas_call(
            functools.partial(kernel, group_size),
            out_shape=(pltpu.VMEM(shape, jnp.float32), pltpu.VMEM((group_size // 2, 8, LANES), jnp.float32)),
            in_specs=[pl.BlockSpec(memory_space=pl.ANY)] * 3,
            out_specs=(pl.BlockSpec(memory_space=pltpu.VMEM), pl.BlockSpec(memory_space=pltpu.VMEM)),
            scratch_shapes=[
                pltpu.VMEM((TOP_BITS, 2, BLOCKS, BLOCK_ROWS, LANES), jnp.float32),
                pltpu.VMEM((2 * LANES, 2 * LANES), jnp.float32),
                pltpu.VMEM((BLOCK_ROWS, BLOCK_ROWS), jnp.float32),
                pltpu.VMEM((CORE, len(SWAP_BLOCKS), HALF, LANES), jnp.float32),
                pltpu.VMEM((HALF, LANES), jnp.float32),
                pltpu.VMEM((HI_BITS + 1, 8, LANES), jnp.float32),
                pltpu.VMEM((TOP_BITS, 8, LANES), jnp.float32),
                pltpu.VMEM((3, 8, LANES), jnp.float32),
                pltpu.SMEM((2, 2, 2, num_qubits), jnp.float32),
                pltpu.SMEM((2, cz_pairs.shape[0]), jnp.int32),
                pltpu.SMEM((cz_pairs.shape[0],), jnp.int32),
                pltpu.SemaphoreType.DMA((2,)),
                pltpu.SemaphoreType.REGULAR((TOP_BITS,)),
                pltpu.SemaphoreType.DMA((4, CORE, len(SWAP_BLOCKS))),
                pltpu.SemaphoreType.DMA((len(LOAD_SPANS),)),
                pltpu.SemaphoreType.DMA((TOP_BITS, 2, MAX_PIECES)),
                pltpu.SemaphoreType.DMA((TOP_BITS, 2, MAX_PIECES)),
                pltpu.SemaphoreType.DMA((group_size,)),
                pltpu.SemaphoreType.DMA((group_size,)),
            ],
            compiler_params=pltpu.CompilerParams(collective_id=0, has_side_effects=True, vmem_limit_bytes=44 * 1024 * 1024),
        )(grid, unitaries.transpose(0, 2, 3, 1), cz_pairs.T)
        state, z_expect = pl.pallas_call(
            functools.partial(flush_kernel, 1.0 / 2 ** num_qubits),
            out_shape=(jax.ShapeDtypeStruct(shape, jnp.float32), jax.ShapeDtypeStruct((1, num_qubits), jnp.float32)),
            in_specs=[pl.BlockSpec(memory_space=pltpu.VMEM)] * 2,
            out_specs=(pl.BlockSpec(memory_space=pl.ANY), pl.BlockSpec(memory_space=pl.ANY)),
            scratch_shapes=[pltpu.VMEM((1, num_qubits), jnp.float32), pltpu.SemaphoreType.DMA((QUARTERS, FLUSH_PIECES)), pltpu.SemaphoreType.DMA],
            compiler_params=pltpu.CompilerParams(vmem_limit_bytes=2 ** 20),
        )(pltpu.with_memory_space_constraint(state, pltpu.VMEM), pltpu.with_memory_space_constraint(parts, pltpu.VMEM))
        state = state.reshape(row_count, 2, LANES).transpose(1, 0, 2).reshape(2, local_size)
        return state, z_expect.reshape(num_qubits)

    return jax.shard_map(local_layer, mesh=mesh, in_specs=(P(None, 'q'), P(), P()), out_specs=(P(None, 'q'), P()), check_vma=False)
```
